8 devices in a mesh: graph: 1 (over z), col: 2 (over y), row: 4 (over x, core).
Axes of the slice: x: 2, y: 2, z: 1, core: 2. Of those that a mesh axis runs over, the one named last changes fastest.
Arguments:
- flow_init: float32 [4096, 4096], P(('graph', 'row'), 'col')
- flow_graph: float32 [4096, 4096], P(('graph', 'row'), 'col')
Outputs:
- output: float32 [4096, 4096], P(('graph', 'row'), 'col')
All inputs are finite; a program needn't handle non-finite values.
Results may differ from the reference program's by a relative error of at most 0.001.
Values are sent between devices in bfloat16 or wider.
A program may use at most 1 GiB of HBM per device.

```python
import jax
import jax.numpy as jnp
from jax import lax

N = 4096
ITERATIONS = 3


def draw_flow(key, floor_level):
    key_width, key_noise = jax.random.split(key)
    node_index = jnp.arange(N, dtype=jnp.float32)
    band_width = N * jax.random.uniform(key_width, (N,), minval=0.01, maxval=0.15)
    raw_offset = jnp.abs(node_index[:, None] - node_index[None, :])
    cyclic_dist = jnp.minimum(raw_offset, N - raw_offset)
    noise_fac = jax.random.uniform(key_noise, (N, N), minval=0.5, maxval=1.5)
    weight = (floor_level + jnp.exp(-cyclic_dist / band_width[None, :])) * noise_fac
    return weight / jnp.sum(weight, axis=0, keepdims=True)


def setup_inputs(seed: int = 0, part: int = 0) -> dict:
    key = jax.random.fold_in(jax.random.key(seed), part)
    key_init, key_graph = jax.random.split(key)
    flow_init = N * draw_flow(key_init, 0.05)
    flow_graph = draw_flow(key_graph, 0.1)
    return {"flow_init": flow_init.astype(jnp.float32), "flow_graph": flow_graph.astype(jnp.float32)}


def reference(flow_init, flow_graph):
    graph_bf = flow_graph.astype(jnp.bfloat16)

    def iteration(flow_cur, unused):
        expanded = jnp.dot(flow_cur.astype(jnp.bfloat16), graph_bf, preferred_element_type=jnp.float32)
        inflated = expanded * expanded
        col_sum = jnp.sum(inflated, axis=0)
        return inflated * (N / col_sum), None

    flow_out, _ = lax.scan(iteration, flow_init, None, length=ITERATIONS)
    return flow_out
```

```python
import functools

import jax
import jax.numpy as jnp
from jax import lax
from jax.experimental import pallas as pl
from jax.experimental.pallas import tpu as pltpu
from jax.sharding import PartitionSpec as P

MESH = pl.DeviceIdType.MESH
WIDTH = 256
PIECES = 2
TILE_M = 512
F32, BF16 = jnp.float32, jnp.bfloat16


def dot(a, b):
    return jnp.dot(a, b, preferred_element_type=F32)


def kernel(n_all, flow_ref, graph_ref, out_ref, sum_ref, g_ref,
           a0, a1, c1, mbuf, gcol, gt, gsend, sums, s1, s2,
           stage_sem, keep_sem, col_sem, gt_sem, out_sem,
           xown_r, xfwd_r, ya_r, yg_r, core_r, sum_r, s1_r, s2_r,
           xown_s, xfwd_s, ya_s, yg_s, cown_s, cfwd_s, sum_s, s1_s, s2_s):
    rows, cols = flow_ref.shape
    nh = cols // WIDTH
    depth = 4 * rows
    half = depth // 2
    kg_rows = 2 * WIDTH
    prow = rows // PIECES

    y = lax.axis_index("col")
    r = lax.axis_index("row")
    z = lax.axis_index("graph")
    x = lax.div(r, 2)
    c = lax.rem(r, 2)
    xn = (z, y, (1 - x) * 2 + c)
    yn = (z, 1 - y, r)
    cn = (z, y, x * 2 + 1 - c)
    dn = (z, y, (1 - x) * 2 + 1 - c)
    lx = x + y - 2 * x * y
    own = pl.multiple_of((lx * 2 + c) * rows, rows)
    oth = pl.multiple_of(((1 - lx) * 2 + c) * rows, rows)

    def remote(src, dst, send, recv, dev):
        return pltpu.make_async_remote_copy(
            src_ref=src, dst_ref=dst, send_sem=send, recv_sem=recv, device_id=dev, device_id_type=MESH)

    def stage_copy(k):
        src = graph_ref if k < nh else flow_ref
        j = k % nh
        return pltpu.make_async_copy(src.at[:, pl.ds(j * WIDTH, WIDTH)], c1.at[k], stage_sem.at[k])

    for j in range(nh):
        stage_copy(j).start()
        stage_copy(nh + j).start()

    bar = pltpu.get_barrier_semaphore()
    for dev in (xn, yn, cn, dn):
        pl.semaphore_signal(bar, inc=1, device_id=dev, device_id_type=MESH)
    pl.semaphore_wait(bar, 4)

    def send_own(j):
        mine = pl.ds(own, rows)
        remote(gsend.at[j], g_ref.at[j, mine], xown_s, xown_r.at[j], xn).start()
        piece = pl.ds(j * WIDTH, WIDTH)
        remote(a0.at[:, piece], a0.at[:, pl.ds(cols + j * WIDTH, WIDTH)], ya_s, ya_r, yn).start()
        remote(gsend.at[j], g_ref.at[j, mine], cown_s, core_r.at[j], cn).start()
        pltpu.make_async_copy(gsend.at[j], g_ref.at[j, mine], keep_sem).start()

    for j in range(nh):
        stage_copy(j).wait()
        gsend[j] = c1[j].astype(BF16)
        stage_copy(nh + j).wait()
        a0[:, pl.ds(j * WIDTH, WIDTH)] = c1[nh + j].astype(BF16)
        if j >= 1:
            send_own(j - 1)
    send_own(nh - 1)
    for j in range(nh):
        for p in range(PIECES):
            src = gsend.at[j, pl.ds(p * prow, prow)]
            dst = g_ref.at[nh + j, pl.ds(oth + p * prow, prow)]
            remote(src, dst, yg_s, yg_r.at[j, p], yn).start()

    pltpu.make_async_copy(gsend, gsend, keep_sem).wait()

    def relay_y(j, p):
        piece = g_ref.at[nh + j, pl.ds(own + p * prow, prow)]
        remote(piece, piece, yg_s, yg_r.at[j, p], yn).wait_recv()
        remote(piece, piece, xfwd_s, xfwd_r.at[j, p], xn).start()
        remote(piece, piece, cfwd_s, core_r.at[nh + j], cn).start()

    def relay_x(j, p):
        piece = g_ref.at[nh + j, pl.ds(oth + p * prow, prow)]
        remote(piece, piece, xfwd_s, xfwd_r.at[j, p], xn).wait_recv()
        remote(piece, piece, cfwd_s, core_r.at[nh + j], cn).start()

    def wait_core(q):
        both = g_ref.at[q, pl.ds(0, half)]
        remote(both, both, cfwd_s, core_r.at[q], cn).wait_recv()

    def col_copy(q):
        slot = lax.rem(q, 2)
        return pltpu.make_async_copy(g_ref.at[q], gcol.at[slot], col_sem.at[slot])

    def tile_copy(kg, n):
        src = g_ref.at[n, pl.ds(pl.multiple_of(kg * kg_rows, kg_rows), kg_rows)]
        return pltpu.make_async_copy(src, gt.at[n], gt_sem.at[n])

    m_tiles = rows // TILE_M

    def over_m(body):
        def go(i, carry):
            body(pl.ds(pl.multiple_of(i * TILE_M, TILE_M), TILE_M))
            return carry
        lax.fori_loop(0, m_tiles, go, 0)

    def first_half(q):
        wait_core(q)
        col_copy(q).start()
        col_copy(q).wait()
        slot = lax.rem(q, 2)

        def body(m):
            c1[q, m, :] = dot(a0[m, :cols], gcol[slot, :half, :])
        over_m(body)

    def early(j, carry):
        piece = g_ref.at[j, pl.ds(oth, rows)]
        remote(piece, piece, xown_s, xown_r.at[j], xn).wait_recv()
        remote(piece, piece, cfwd_s, core_r.at[j], cn).start()

        @pl.when(j >= 1)
        def _():
            first_half(j - 1)
        return carry
    lax.fori_loop(0, nh, early, 0)
    first_half(nh - 1)

    other_a = a0.at[:, pl.ds(cols, cols)]
    remote(other_a, other_a, ya_s, ya_r, yn).wait_recv()

    def add_product(kg, n, g_tile):
        k = pl.ds(pl.multiple_of(kg * kg_rows, kg_rows), kg_rows)

        @pl.when(kg == 0)
        def _():
            c1[n] = dot(a1[:, k], g_tile[...])

        @pl.when(kg > 0)
        def _():
            c1[n] += dot(a1[:, k], g_tile[...])

    def col_tile(slot, kg):
        return gcol.at[slot, pl.ds(pl.multiple_of(kg * kg_rows, kg_rows), kg_rows)]

    def step(q, first, relay):
        slot = lax.rem(q, 2)
        kg = lax.div(q, 2)
        odd = lax.rem(q, 2) == 1

        @pl.when(odd)
        def _():
            lax.fori_loop(0, q, lambda n, t: (tile_copy(kg, n).start(), t)[1], 0)

        sums[q, r] = jnp.zeros((8, WIDTH), F32)

        def body(m):
            if first:
                v = c1[q, m, :] + dot(a0[m, cols:], gcol[slot, half:, :])
            else:
                v = dot(a0[m, :], gcol[slot])
            v = v * v
            mbuf[0, m, :] = v
            sums[q, r] += jnp.broadcast_to(jnp.sum(v, axis=0, keepdims=True), (8, WIDTH))
        over_m(body)

        for dev in (cn, xn, dn):
            remote(sums.at[q, r], sums.at[q, r], sum_s, sum_r.at[q], dev).start()

        def left(k, carry):
            add_product(k, q, col_tile(slot, k))
            return carry
        lax.fori_loop(0, kg, left, 0)

        relay()

        three = sums.at[q, pl.ds(0, 3)]
        remote(three, three, sum_s, sum_r.at[q], cn).wait_recv()
        total = (sums[q, 0] + sums[q, 1]) + (sums[q, 2] + sums[q, 3])
        scale = (n_all / total)[:1]
        a1[:, pl.ds(pl.multiple_of(q * WIDTH, WIDTH), WIDTH)] = (mbuf[0] * scale).astype(BF16)

        @pl.when(odd)
        def _():
            def right(n, carry):
                tile_copy(kg, n).wait()
                add_product(kg, n, gt.at[n])
                return carry
            lax.fori_loop(0, q, right, 0)
            add_product(kg, q, col_tile(slot, kg))

    col_copy(0).start()

    def own_step(q, carry):
        col_copy(q).wait()

        @pl.when(q + 1 < nh)
        def _():
            col_copy(q + 1).start()

        def relay():
            @pl.when(q == 2)
            def _():
                relay_y(0, 0)

            @pl.when(q == 4)
            def _():
                relay_y(0, 1)

            @pl.when(q == 6)
            def _():
                relay_y(1, 0)
                relay_x(0, 0)
        step(q, True, relay)
        return carry
    lax.fori_loop(0, nh, own_step, 0)

    def other_step(j, carry):
        q = nh + j

        @pl.when(j + 1 < nh)
        def _():
            relay_y(j + 1, 1)
        relay_x(j, 1)
        wait_core(q)
        col_copy(q).start()
        col_copy(q).wait()

        def relay():
            @pl.when(j + 2 < nh)
            def _():
                relay_y(j + 2, 0)

            @pl.when(j + 1 < nh)
            def _():
                relay_x(j + 1, 0)
        step(q, False, relay)
        return carry
    lax.fori_loop(0, nh, other_step, 0)

    col_copy(0).start()

    def square(n, carry):
        v = c1[n]
        v = v * v
        c1[n] = v
        s1[r, pl.ds(n, 1), :] = jnp.sum(v, axis=0, keepdims=True)
        return carry
    lax.fori_loop(0, 2 * nh, square, 0)
    for dev in (cn, xn, dn):
        remote(s1.at[r], s1.at[r], s1_s, s1_r, dev).start()
    remote(a0.at[:, pl.ds(0, cols)], a0.at[:, pl.ds(0, cols)], ya_s, ya_r, yn).wait_send()
    three = s1.at[pl.ds(0, 3)]
    remote(three, three, s1_s, s1_r, cn).wait_recv()

    def rescale(n, carry):
        line = pl.ds(n, 1)
        total = (s1[0, line, :] + s1[1, line, :]) + (s1[2, line, :] + s1[3, line, :])
        a0[:, pl.ds(pl.multiple_of(n * WIDTH, WIDTH), WIDTH)] = (c1[n] * (n_all / total)).astype(BF16)
        return carry
    lax.fori_loop(0, 2 * nh, rescale, 0)

    def out_copy(n):
        slot = lax.rem(n, 2)
        dst = out_ref.at[:, pl.ds(pl.multiple_of(n * WIDTH, WIDTH), WIDTH)]
        return pltpu.make_async_copy(mbuf.at[slot], dst, out_sem.at[slot])

    def last(n, carry):
        slot = lax.rem(n, 2)
        col_copy(n).wait()

        @pl.when(n + 1 < nh)
        def _():
            col_copy(n + 1).start()

        @pl.when(n >= 2)
        def _():
            out_copy(n - 2).wait()
        s2[r, pl.ds(n, 1), :] = jnp.zeros((1, WIDTH), F32)

        def body(m):
            v = dot(a0[m, :], gcol[slot])
            v = v * v
            mbuf[slot, m, :] = v
            s2[r, pl.ds(n, 1), :] += jnp.sum(v, axis=0, keepdims=True)
        over_m(body)
        out_copy(n).start()
        return carry
    lax.fori_loop(0, nh, last, 0)

    for dev in (cn, xn, dn):
        remote(s2.at[r], s2.at[r], s2_s, s2_r, dev).start()
    out_copy(nh - 2).wait()
    out_copy(nh - 1).wait()
    three = s2.at[pl.ds(0, 3)]
    remote(three, three, s2_s, s2_r, cn).wait_recv()
    sum_ref[...] = (s2[0] + s2[1]) + (s2[2] + s2[3])

    remote(gsend, gsend, xown_s, xown_r.at[0], xn).wait_send()
    remote(gsend, gsend, yg_s, xown_r.at[0], yn).wait_send()
    remote(gsend, gsend, cown_s, xown_r.at[0], cn).wait_send()
    fwd = g_ref.at[pl.ds(0, nh), pl.ds(0, rows)]
    remote(fwd, fwd, xfwd_s, xown_r.at[0], xn).wait_send()
    fwd = g_ref.at[pl.ds(0, nh), pl.ds(0, 3 * rows)]
    remote(fwd, fwd, cfwd_s, xown_r.at[0], cn).wait_send()
    part = sums.at[:, pl.ds(0, 3)]
    remote(part, part, sum_s, xown_r.at[0], cn).wait_send()
    remote(s1.at[pl.ds(0, 3)], s1.at[pl.ds(0, 3)], s1_s, xown_r.at[0], cn).wait_send()
    remote(s2.at[pl.ds(0, 3)], s2.at[pl.ds(0, 3)], s2_s, xown_r.at[0], cn).wait_send()


def solution(mesh):
    block_spec = P(("graph", "row"), "col")

    def device_step(init_blk, graph_blk):
        rows, cols = init_blk.shape
        n_all = 2 * cols
        nh = cols // WIDTH
        dma = pltpu.SemaphoreType.DMA
        any_spec = pl.BlockSpec(memory_space=pl.ANY)
        raw, col_sum, _ = pl.pallas_call(
            functools.partial(kernel, float(n_all)),
            out_shape=(
                jax.ShapeDtypeStruct((rows, cols), F32),
                jax.ShapeDtypeStruct((nh, WIDTH), F32),
                jax.ShapeDtypeStruct((2 * nh, n_all, WIDTH), BF16),
            ),
            in_specs=[any_spec, any_spec],
            out_specs=(any_spec, pl.BlockSpec(memory_space=pltpu.VMEM), any_spec),
            scratch_shapes=[
                pltpu.VMEM((rows, n_all), BF16),
                pltpu.VMEM((rows, n_all), BF16),
                pltpu.VMEM((2 * nh, rows, WIDTH), F32),
                pltpu.VMEM((2, rows, WIDTH), F32),
                pltpu.VMEM((2, n_all, WIDTH), BF16),
                pltpu.VMEM((2 * nh, 2 * WIDTH, WIDTH), BF16),
                pltpu.VMEM((nh, rows, WIDTH), BF16),
                pltpu.VMEM((2 * nh, 4, 8, WIDTH), F32),
                pltpu.VMEM((4, 2 * nh, WIDTH), F32),
                pltpu.VMEM((4, nh, WIDTH), F32),
                dma((2 * nh,)), dma, dma((2,)), dma((2 * nh,)), dma((2,)),
                dma((nh,)), dma((nh, PIECES)), dma, dma((nh, PIECES)), dma((2 * nh,)), dma((2 * nh,)), dma, dma,
                dma, dma, dma, dma, dma, dma, dma, dma, dma,
            ],
            compiler_params=pltpu.CompilerParams(
                collective_id=0, has_side_effects=True, vmem_limit_bytes=62 * 2**20),
            name="mcl",
        )(init_blk, graph_blk)
        return raw * (n_all / col_sum.reshape(cols))

    return jax.shard_map(device_step, mesh=mesh, in_specs=(block_spec, block_spec), out_specs=block_spec, check_vma=False)
```

```python
import contextlib
import functools

import jax
import jax.numpy as jnp
from jax import lax
from jax.experimental import pallas as pl
from jax.experimental.pallas import tpu as pltpu
from jax.sharding import PartitionSpec as P

MESH = pl.DeviceIdType.MESH
WIDTH = 256
PIECES = 4
F32, BF16 = jnp.float32, jnp.bfloat16


def nothing(name):
    return contextlib.nullcontext()


scope = nothing


def dot(a, b):
    return jnp.dot(a, b, preferred_element_type=F32)


def kernel(n_all, flow_ref, graph_ref, out_ref, sum_ref, g_ref,
           a0, a1, c1, mbuf, gown, gcol, gt, sums, s1, s2,
           stage_sem, col_sem, gt_sem, out_sem,
           xown_r, xfwd_r, ya_r, yg_r, core_r, sum_r, s1_r, s2_r,
           xown_s, xfwd_s, ya_s, yg_s, cown_s, cfwd_s, sum_s, s1_s, s2_s):
    rows, cols = flow_ref.shape
    nh = cols // WIDTH
    depth = 4 * rows
    half = depth // 2
    quad = half // 2
    kg_rows = 2 * WIDTH
    prow = rows // PIECES

    y = lax.axis_index("col")
    r = lax.axis_index("row")
    z = lax.axis_index("graph")
    x = lax.div(r, 2)
    c = lax.rem(r, 2)
    xn = (z, y, (1 - x) * 2 + c)
    yn = (z, 1 - y, r)
    cn = (z, y, x * 2 + 1 - c)
    dn = (z, y, (1 - x) * 2 + 1 - c)
    lx = x + y - 2 * x * y
    own = pl.multiple_of((lx * 2 + c) * rows, rows)
    oth = pl.multiple_of(((1 - lx) * 2 + c) * rows, rows)
    mine, theirs = pl.ds(own, rows), pl.ds(oth, rows)

    def remote(src, dst, send, recv, dev):
        return pltpu.make_async_remote_copy(
            src_ref=src, dst_ref=dst, send_sem=send, recv_sem=recv, device_id=dev, device_id_type=MESH)

    def chunk(q):
        return pl.ds(pl.multiple_of(q * WIDTH, WIDTH), WIDTH)

    def stage_copy(k):
        src = graph_ref if k < nh else flow_ref
        return pltpu.make_async_copy(src.at[:, pl.ds((k % nh) * WIDTH, WIDTH)], c1.at[k], stage_sem.at[k])

    def stage(j):
        if j < nh:
            stage_copy(j).start()
            stage_copy(nh + j).start()

    stage(0)
    bar = pltpu.get_barrier_semaphore()
    for dev in (xn, yn, cn, dn):
        pl.semaphore_signal(bar, inc=1, device_id=dev, device_id_type=MESH)
    stage(1)
    stage(2)

    def send_own(j):
        block = gown.at[j, mine]
        remote(block, block, xown_s, xown_r.at[j], xn).start()
        piece = pl.ds(j * WIDTH, WIDTH)
        remote(a0.at[:, piece], a0.at[:, pl.ds(cols + j * WIDTH, WIDTH)], ya_s, ya_r.at[j * 2 // nh], yn).start()
        remote(block, block, cown_s, core_r.at[j], cn).start()

    for j in range(nh):
        with scope("cast"):
            stage_copy(j).wait()
            gown[j, mine, :] = c1[j].astype(BF16)
            stage_copy(nh + j).wait()
            a0[:, pl.ds(j * WIDTH, WIDTH)] = c1[nh + j].astype(BF16)
            stage(j + 3)
            if j == 1:
                pl.semaphore_wait(bar, 4)
            if j >= 1:
                send_own(j - 1)
    send_own(nh - 1)
    for j in range(nh):
        for p in range(PIECES):
            src = gown.at[j, pl.ds(own + p * prow, prow)]
            dst = g_ref.at[j, pl.ds(oth + p * prow, prow)]
            remote(src, dst, yg_s, yg_r.at[j, p], yn).start()

    n_pieces = nh * PIECES

    def relay(k, offset, sem, recv, dev, forward):
        @pl.when((k >= 0) & (k < n_pieces))
        def _():
            j, p = lax.div(k, PIECES), lax.rem(k, PIECES)
            piece = g_ref.at[j, pl.ds(pl.multiple_of(offset + p * prow, prow), prow)]
            remote(piece, piece, sem, recv.at[j, p], dev).wait_recv()
            if forward:
                remote(piece, piece, xfwd_s, xfwd_r.at[j, p], xn).start()
            remote(piece, piece, cfwd_s, core_r.at[nh + j], cn).start()

    def relay_y(*ks):
        for k in ks:
            with scope("relay_y"):
                relay(jnp.int32(k), own, yg_s, yg_r, yn, True)

    def relay_x(*ks):
        for k in ks:
            with scope("relay_x"):
                relay(jnp.int32(k), oth, xfwd_s, xfwd_r, xn, False)

    def wait_core(q):
        with scope("wait_core"):
            both = gown.at[0, pl.ds(0, half)]
            remote(both, both, cfwd_s, core_r.at[q], cn).wait_recv()

    def col_copy(q):
        slot = lax.rem(q, 2)
        return pltpu.make_async_copy(g_ref.at[q - nh], gcol.at[slot], col_sem.at[slot])

    def k_rows(kg):
        return pl.ds(pl.multiple_of(kg * kg_rows, kg_rows), kg_rows)

    def tile_copy(kg, j):
        return pltpu.make_async_copy(g_ref.at[j, k_rows(kg)], gt.at[j], gt_sem.at[j])

    def loop(lo, hi, body):
        def go(i, carry):
            body(i)
            return carry
        lax.fori_loop(lo, hi, go, 0)

    def unrolled(n, width, body):
        def some(i):
            for t in range(width):
                body(i * width + t)
        loop(0, n, some)

    def first_half(q):
        wait_core(q)

        c1[q] = dot(a0[:, :cols], gown[q, :half, :])

    def third_quarter(q):
        c1[q] += dot(a0[:, cols:cols + quad], gown[q, half:half + quad, :])

    def wait_a(i):
        with scope("wait_a"):
            part = a0.at[:, pl.ds(0, quad)]
            remote(part, part, ya_s, ya_r.at[i], yn).wait_recv()

    def early(j):
        with scope("wait_xown"):
            block = gown.at[j, theirs]
            remote(block, block, xown_s, xown_r.at[j], xn).wait_recv()
        remote(block, block, cfwd_s, core_r.at[j], cn).start()

        @pl.when(j >= 1)
        def _():
            with scope("first_half"):
                first_half(j - 1)

        @pl.when(j == nh - 3)
        def _():
            wait_a(0)

        @pl.when(j >= nh - 3)
        def _():
            with scope("third_quarter"):
                first = 2 * (j - (nh - 3))
                third_quarter(first)
                third_quarter(first + 1)
    loop(0, nh, early)
    with scope("early_end"):
        third_quarter(nh - 2)
        first_half(nh - 1)
        third_quarter(nh - 1)
    wait_a(1)

    def add_product(kg, n, g_tile):
        @pl.when(kg == 0)
        def _():
            c1[n] = dot(a1[:, k_rows(kg)], g_tile[...])

        @pl.when(kg > 0)
        def _():
            c1[n] += dot(a1[:, k_rows(kg)], g_tile[...])

    def finish(q):
        with scope("finish"):
            three = sums.at[q, pl.ds(0, 3)]
            remote(three, three, sum_s, sum_r.at[q], cn).wait_recv()
            total = (sums[q, 0] + sums[q, 1]) + (sums[q, 2] + sums[q, 3])
            scale = (n_all / total)[:1]
            a1[:, chunk(q)] = (mbuf[lax.rem(q, 2)] * scale).astype(BF16)

    def step(q, first, after_first, after_left):
        slot = lax.rem(q, 2)
        done = lax.div(q, 2)
        even = slot == 0

        if not first:
            @pl.when(even)
            def _():
                loop(0, q - nh, lambda j: tile_copy(done - 1, j).start())

        with scope("c0"):
            if first:
                v = c1[q] + dot(a0[:, cols + quad:], gown[q, half + quad:, :])
            else:
                v = dot(a0[...], gcol[slot])
            v = v * v
            mbuf[slot] = v
            sums[q, r] = jnp.broadcast_to(jnp.sum(v, axis=0, keepdims=True), (8, WIDTH))
        for dev in (cn, xn, dn):
            remote(sums.at[q, r], sums.at[q, r], sum_s, sum_r.at[q], dev).start()

        after_first()

        @pl.when(q >= 1)
        def _():
            finish(q - 1)

        with scope("left"):
            if first:
                loop(0, done, lambda k: add_product(k, q, gown.at[q, k_rows(k)]))
            else:
                c1[q] = dot(a1[:, :cols], gcol[slot, :half, :])
                loop(nh // 2, done, lambda k: add_product(k, q, gcol.at[slot, k_rows(k)]))

        after_left()

        @pl.when(even & (q >= 2))
        def _():
            with scope("right"):
                kg = done - 1
                if first:
                    def pair(i):
                        for n in (2 * i, 2 * i + 1):
                            c1[n] += dot(a1[:, k_rows(kg)], gown[n, k_rows(kg), :])

                    @pl.when(kg == 0)
                    def _():
                        for n in (0, 1):
                            c1[n] = dot(a1[:, k_rows(0)], gown[n, k_rows(0), :])

                    @pl.when(kg > 0)
                    def _():
                        loop(0, done, pair)
                else:
                    def some(i):
                        for n in range(4):
                            c1[4 * i + n] += dot(a1[:, k_rows(kg)], gown[4 * i + n, k_rows(kg), :])
                    loop(0, nh // 4, some)

                    def pair(i):
                        for j in (2 * i, 2 * i + 1):
                            tile_copy(kg, j).wait()
                        for j in (2 * i, 2 * i + 1):
                            c1[nh + j] += dot(a1[:, k_rows(kg)], gt[j])
                    loop(0, done - nh // 2, pair)

    def own_step(q):
        def after_first():
            for at, ys, xs in ((1, (0,), ()), (2, (1,), ()), (4, (2,), ()), (5, (3,), (0, 1)), (6, (4,), ()), (7, (5,), (2,))):
                @pl.when(q == at)
                def _():
                    relay_y(*ys)
                    relay_x(*xs)
        step(q, True, after_first, lambda: None)
    loop(0, nh, own_step)
    relay_y(6)
    relay_x(3)
    wait_core(nh)
    col_copy(nh).start()

    def other_step(j):
        q = nh + j
        k = PIECES * j
        with scope("load"):
            col_copy(q).wait()

        def after_first():
            relay_y(k + 7)
            relay_x(k + 4, k + 5)

        def after_left():
            relay_y(k + 8)
            relay_x(k + 6)
        step(q, False, after_first, after_left)
        relay_y(k + 9)
        relay_x(k + 7)

        @pl.when(j + 1 < nh)
        def _():
            wait_core(q + 1)
            col_copy(q + 1).start()
        relay_y(k + 10)
    loop(0, nh, other_step)

    last_kg = nh - 1
    loop(0, nh, lambda j: tile_copy(last_kg, j).start())
    finish(2 * nh - 1)

    def close(n, g_tile):
        v = c1[n] + dot(a1[:, k_rows(last_kg)], g_tile[...])
        v = v * v
        c1[n] = v
        s1[r, pl.ds(n, 1), :] = jnp.sum(v, axis=0, keepdims=True)

    def close_other(j):
        tile_copy(last_kg, j).wait()
        close(nh + j, gt.at[j])
    with scope("close"):
        unrolled(nh // 4, 4, lambda n: close(n, gown.at[n, k_rows(last_kg)]))
        unrolled(nh // 4, 4, close_other)
    for dev in (cn, xn, dn):
        remote(s1.at[r], s1.at[r], s1_s, s1_r, dev).start()
    with scope("wait_s1"):
        remote(a0.at[:, pl.ds(0, cols)], a0.at[:, pl.ds(0, cols)], ya_s, ya_r.at[0], yn).wait_send()
        three = s1.at[pl.ds(0, 3)]
        remote(three, three, s1_s, s1_r, cn).wait_recv()

    def rescale(n):
        line = pl.ds(n, 1)
        total = (s1[0, line, :] + s1[1, line, :]) + (s1[2, line, :] + s1[3, line, :])
        a0[:, chunk(n)] = (c1[n] * (n_all / total)).astype(BF16)
    with scope("rescale"):
        loop(0, 2 * nh, rescale)

    def out_copy(n):
        slot = lax.rem(n, 2)
        return pltpu.make_async_copy(mbuf.at[slot], out_ref.at[:, chunk(n)], out_sem.at[slot])

    def last(n):
        slot = lax.rem(n, 2)

        @pl.when(n >= 2)
        def _():
            out_copy(n - 2).wait()
        v = dot(a0[...], gown[n])
        v = v * v
        mbuf[slot] = v
        s2[r, pl.ds(n, 1), :] = jnp.sum(v, axis=0, keepdims=True)
        out_copy(n).start()
    with scope("last"):
        loop(0, nh, last)

    for dev in (cn, xn, dn):
        remote(s2.at[r], s2.at[r], s2_s, s2_r, dev).start()

    def sent(ref, sem):
        remote(ref, ref, sem, s2_r, cn).wait_send()
    sent(gown.at[:, pl.ds(0, rows)], xown_s)
    sent(gown.at[:, pl.ds(0, rows)], yg_s)
    sent(gown.at[:, pl.ds(0, rows)], cown_s)
    sent(gown.at[:, pl.ds(0, rows)], xfwd_s)
    sent(gown.at[:, pl.ds(0, 3 * rows)], cfwd_s)
    sent(sums.at[:, pl.ds(0, 3)], sum_s)
    sent(s1.at[pl.ds(0, 3)], s1_s)
    out_copy(nh - 2).wait()
    out_copy(nh - 1).wait()
    with scope("wait_s2"):
        three = s2.at[pl.ds(0, 3)]
        remote(three, three, s2_s, s2_r, cn).wait()
    sum_ref[...] = (s2[0] + s2[1]) + (s2[2] + s2[3])


def solution(mesh):
    block_spec = P(("graph", "row"), "col")

    def device_step(init_blk, graph_blk):
        rows, cols = init_blk.shape
        n_all = 2 * cols
        nh = cols // WIDTH
        dma = pltpu.SemaphoreType.DMA
        any_spec = pl.BlockSpec(memory_space=pl.ANY)
        raw, col_sum, _ = pl.pallas_call(
            functools.partial(kernel, float(n_all)),
            out_shape=(
                jax.ShapeDtypeStruct((rows, cols), F32),
                jax.ShapeDtypeStruct((nh, WIDTH), F32),
                jax.ShapeDtypeStruct((nh, n_all, WIDTH), BF16),
            ),
            in_specs=[any_spec, any_spec],
            out_specs=(any_spec, pl.BlockSpec(memory_space=pltpu.VMEM), any_spec),
            scratch_shapes=[
                pltpu.VMEM((rows, n_all), BF16),
                pltpu.VMEM((rows, n_all), BF16),
                pltpu.VMEM((2 * nh, rows, WIDTH), F32),
                pltpu.VMEM((2, rows, WIDTH), F32),
                pltpu.VMEM((nh, n_all, WIDTH), BF16),
                pltpu.VMEM((2, n_all, WIDTH), BF16),
                pltpu.VMEM((nh, 2 * WIDTH, WIDTH), BF16),
                pltpu.VMEM((2 * nh, 4, 8, WIDTH), F32),
                pltpu.VMEM((4, 2 * nh, WIDTH), F32),
                pltpu.VMEM((4, nh, WIDTH), F32),
                dma((2 * nh,)), dma((2,)), dma((nh,)), dma((2,)),
                dma((nh,)), dma((nh, PIECES)), dma((2,)), dma((nh, PIECES)), dma((2 * nh,)), dma((2 * nh,)), dma, dma,
                dma, dma, dma, dma, dma, dma, dma, dma, dma,
            ],
            compiler_params=pltpu.CompilerParams(
                collective_id=0, has_side_effects=True, vmem_limit_bytes=62 * 2**20),
            name="mcl",
        )(init_blk, graph_blk)
        return raw * (n_all / col_sum.reshape(cols))

    return jax.shard_map(device_step, mesh=mesh, in_specs=(block_spec, block_spec), out_specs=block_spec, check_vma=False)
```

```python
import contextlib
import functools

import jax
import jax.numpy as jnp
from jax import lax
from jax.experimental import pallas as pl
from jax.experimental.pallas import tpu as pltpu
from jax.sharding import PartitionSpec as P

MESH = pl.DeviceIdType.MESH
WIDTH = 256
PIECES = 4
TILE_M = 512
F32, BF16 = jnp.float32, jnp.bfloat16


def nothing(name):
    return contextlib.nullcontext()


scope = nothing


def dot(a, b):
    return jnp.dot(a, b, preferred_element_type=F32)


def kernel(n_all, flow_ref, graph_ref, out_ref, sum_ref, g_ref,
           a0, a1, a2, c1, mbuf, gown, gcol, gt, sums, s1, s2,
           stage_sem, col_sem, gt_sem, out_sem,
           xown_r, xfwd_r, ya_r, yg_r, y1_r, y2_r, core_r, sum_r, s1_r, s2_r,
           xown_s, xfwd_s, ya_s, yg_s, y1_s, y2_s, cown_s, cfwd_s, cfar_s, sum_s, s1_s, s2_s):
    rows, cols = flow_ref.shape
    nh = cols // WIDTH
    nf = nh - 1
    nc = nh + nf
    depth = 4 * rows
    half = depth // 2
    quad = half // 2
    kg_rows = 2 * WIDTH
    prow = rows // PIECES

    y = lax.axis_index("col")
    r = lax.axis_index("row")
    z = lax.axis_index("graph")
    x = lax.div(r, 2)
    c = lax.rem(r, 2)
    xn = (z, y, (1 - x) * 2 + c)
    yn = (z, 1 - y, r)
    cn = (z, y, x * 2 + 1 - c)
    dn = (z, y, (1 - x) * 2 + 1 - c)
    lx = x + y - 2 * x * y
    own = pl.multiple_of((lx * 2 + c) * rows, rows)
    oth = pl.multiple_of(((1 - lx) * 2 + c) * rows, rows)
    mine, theirs = pl.ds(own, rows), pl.ds(oth, rows)

    def remote(src, dst, send, recv, dev):
        return pltpu.make_async_remote_copy(
            src_ref=src, dst_ref=dst, send_sem=send, recv_sem=recv, device_id=dev, device_id_type=MESH)

    def chunk(q):
        return pl.ds(pl.multiple_of(q * WIDTH, WIDTH), WIDTH)

    def stage_copy(k):
        src = graph_ref if k < nh else flow_ref
        return pltpu.make_async_copy(src.at[:, pl.ds((k % nh) * WIDTH, WIDTH)], c1.at[k], stage_sem.at[k])

    def stage(j):
        if j < nh:
            stage_copy(j).start()
            stage_copy(nh + j).start()

    stage(0)
    bar = pltpu.get_barrier_semaphore()
    for dev in (xn, yn, cn, dn):
        pl.semaphore_signal(bar, inc=1, device_id=dev, device_id_type=MESH)
    stage(1)
    stage(2)

    def send_own(j):
        block = gown.at[j, mine]
        remote(block, block, xown_s, xown_r.at[j], xn).start()
        piece = pl.ds(j * WIDTH, WIDTH)
        remote(a0.at[:, piece], a0.at[:, pl.ds(cols + j * WIDTH, WIDTH)], ya_s, ya_r.at[j * 2 // nh], yn).start()
        remote(block, block, cown_s, core_r.at[j], cn).start()

    for j in range(nh):
        with scope("cast"):
            stage_copy(j).wait()
            gown[j, mine, :] = c1[j].astype(BF16)
            stage_copy(nh + j).wait()
            a0[:, pl.ds(j * WIDTH, WIDTH)] = c1[nh + j].astype(BF16)
            stage(j + 3)
            if j == 1:
                pl.semaphore_wait(bar, 4)
            if j >= 1:
                send_own(j - 1)
    send_own(nh - 1)
    for j in range(nf):
        for p in range(PIECES):
            src = gown.at[j, pl.ds(own + p * prow, prow)]
            dst = g_ref.at[j, pl.ds(oth + p * prow, prow)]
            remote(src, dst, yg_s, yg_r.at[j, p], yn).start()

    n_pieces = nf * PIECES

    def relay(k, offset, sem, recv, dev, forward):
        @pl.when((k >= 0) & (k < n_pieces))
        def _():
            j, p = lax.div(k, PIECES), lax.rem(k, PIECES)
            piece = g_ref.at[j, pl.ds(pl.multiple_of(offset + p * prow, prow), prow)]
            remote(piece, piece, sem, recv.at[j, p], dev).wait_recv()
            if forward:
                remote(piece, piece, xfwd_s, xfwd_r.at[j, p], xn).start()
            remote(piece, piece, cfar_s, core_r.at[nh + j], cn).start()

    def relay_y(*ks):
        for k in ks:
            with scope("relay_y"):
                relay(jnp.int32(k), own, yg_s, yg_r, yn, True)

    def relay_x(*ks):
        for k in ks:
            with scope("relay_x"):
                relay(jnp.int32(k), oth, xfwd_s, xfwd_r, xn, False)

    lent, borrowed = pl.ds((nh - 1) * WIDTH, WIDTH), pl.ds((2 * nh - 1) * WIDTH, WIDTH)

    def wait_core(q):
        with scope("wait_core"):
            both = gown.at[0, pl.ds(0, half)]
            remote(both, both, cfwd_s, core_r.at[q], cn).wait_recv()

    def col_copy(q):
        slot = lax.rem(q, 2)
        return pltpu.make_async_copy(g_ref.at[q - nh], gcol.at[slot], col_sem.at[slot])

    def k_rows(kg):
        return pl.ds(pl.multiple_of(kg * kg_rows, kg_rows), kg_rows)

    def tile_copy(kg, j):
        return pltpu.make_async_copy(g_ref.at[j, k_rows(kg)], gt.at[j], gt_sem.at[j])

    def loop(lo, hi, body):
        def go(i, carry):
            body(i)
            return carry
        lax.fori_loop(lo, hi, go, 0)

    def over_m(body):
        loop(0, rows // TILE_M, lambda i: body(pl.ds(pl.multiple_of(i * TILE_M, TILE_M), TILE_M)))

    def unrolled(n, width, body):
        def some(i):
            for t in range(width):
                body(i * width + t)
        loop(0, n, some)

    def first_half(q):
        wait_core(q)

        c1[q] = dot(a0[:, :cols], gown[q, :half, :])

    def third_quarter(q):
        c1[q] += dot(a0[:, cols:cols + quad], gown[q, half:half + quad, :])

    def wait_a(i):
        with scope("wait_a"):
            part = a0.at[:, pl.ds(0, quad)]
            remote(part, part, ya_s, ya_r.at[i], yn).wait_recv()

    def early(j):
        with scope("wait_xown"):
            block = gown.at[j, theirs]
            remote(block, block, xown_s, xown_r.at[j], xn).wait_recv()
        remote(block, block, cfwd_s, core_r.at[j], cn).start()

        @pl.when(j >= 1)
        def _():
            with scope("first_half"):
                first_half(j - 1)

        @pl.when(j == nh - 3)
        def _():
            wait_a(0)

        @pl.when(j >= nh - 3)
        def _():
            with scope("third_quarter"):
                first = 2 * (j - (nh - 3))
                third_quarter(first)
                third_quarter(first + 1)
    loop(0, nh, early)
    with scope("early_end"):
        third_quarter(nh - 2)
        first_half(nh - 1)
        third_quarter(nh - 1)
    wait_a(1)

    def add_product(kg, n, g_tile):
        @pl.when(kg == 0)
        def _():
            c1[n] = dot(a1[:, k_rows(kg)], g_tile[...])

        @pl.when(kg > 0)
        def _():
            c1[n] += dot(a1[:, k_rows(kg)], g_tile[...])

    def finish(q):
        with scope("finish"):
            three = sums.at[q, pl.ds(0, 3)]
            remote(three, three, sum_s, sum_r.at[q], cn).wait_recv()
            total = (sums[q, 0] + sums[q, 1]) + (sums[q, 2] + sums[q, 3])
            scale = (n_all / total)[:1]
            a1[:, chunk(q)] = (mbuf[lax.rem(q, 2)] * scale).astype(BF16)

    def step(q, first, after_first, after_left):
        slot = lax.rem(q, 2)
        done = lax.div(q, 2)
        even = slot == 0

        if not first:
            @pl.when(even)
            def _():
                loop(0, q - nh, lambda j: tile_copy(done - 1, j).start())

        with scope("c0"):
            if first:
                v = c1[q] + dot(a0[:, cols + quad:], gown[q, half + quad:, :])
                v = v * v
                mbuf[slot] = v
                sums[q, r] = jnp.broadcast_to(jnp.sum(v, axis=0, keepdims=True), (8, WIDTH))
            else:
                sums[q, r] = jnp.zeros((8, WIDTH), F32)

                def body(m):
                    v = dot(a0[m, :], gcol[slot])
                    v = v * v
                    mbuf[slot, m, :] = v
                    sums[q, r] += jnp.broadcast_to(jnp.sum(v, axis=0, keepdims=True), (8, WIDTH))
                over_m(body)
        for dev in (cn, xn, dn):
            remote(sums.at[q, r], sums.at[q, r], sum_s, sum_r.at[q], dev).start()

        after_first()

        @pl.when(q >= 1)
        def _():
            finish(q - 1)

        with scope("left"):
            if first:
                loop(0, done, lambda k: add_product(k, q, gown.at[q, k_rows(k)]))
            else:
                def body(m):
                    c1[q, m, :] = dot(a1[m, :cols], gcol[slot, :half, :])
                over_m(body)
                loop(nh // 2, done, lambda k: add_product(k, q, gcol.at[slot, k_rows(k)]))

        after_left()

        @pl.when(even & (q >= 2))
        def _():
            with scope("right"):
                kg = done - 1
                if first:
                    def pair(i):
                        for n in (2 * i, 2 * i + 1):
                            c1[n] += dot(a1[:, k_rows(kg)], gown[n, k_rows(kg), :])

                    @pl.when(kg == 0)
                    def _():
                        for n in (0, 1):
                            c1[n] = dot(a1[:, k_rows(0)], gown[n, k_rows(0), :])

                    @pl.when(kg > 0)
                    def _():
                        loop(0, done, pair)
                else:
                    def some(i):
                        for n in range(4):
                            c1[4 * i + n] += dot(a1[:, k_rows(kg)], gown[4 * i + n, k_rows(kg), :])
                    loop(0, nh // 4, some)

                    def pair(i):
                        for j in (2 * i, 2 * i + 1):
                            tile_copy(kg, j).wait()
                        for j in (2 * i, 2 * i + 1):
                            c1[nh + j] += dot(a1[:, k_rows(kg)], gt[j])
                    loop(0, done - nh // 2, pair)

    def own_step(q):
        def after_first():
            for at, ys, xs in ((1, (0,), ()), (2, (1,), ()), (4, (2,), ()), (5, (3,), (0, 1)), (6, (4,), ()), (7, (5,), (2,))):
                @pl.when(q == at)
                def _():
                    relay_y(*ys)
                    relay_x(*xs)
        step(q, True, after_first, lambda: None)
    loop(0, nh, own_step)
    relay_y(6)
    relay_x(3)
    wait_core(nh)
    col_copy(nh).start()

    def other_step(j):
        q = nh + j
        k = PIECES * j
        with scope("load"):
            col_copy(q).wait()

        def after_first():
            relay_y(k + 7)
            relay_x(k + 4, k + 5)

        def after_left():
            @pl.when(j == 0)
            def _():
                remote(a1.at[:, lent], a1.at[:, borrowed], y1_s, y1_r, yn).start()
            relay_y(k + 8)
            relay_x(k + 6)
        step(q, False, after_first, after_left)
        relay_y(k + 9)
        relay_x(k + 7)

        @pl.when(j + 1 < nf)
        def _():
            wait_core(q + 1)
            col_copy(q + 1).start()
        relay_y(k + 10)
    loop(0, nf, other_step)

    last_kg = nh - 1
    loop(0, nf, lambda j: tile_copy(last_kg, j).start())
    s1[r] = jnp.zeros((2 * nh, WIDTH), F32)
    finish(nc - 1)
    with scope("wait_a1"):
        remote(a1.at[:, lent], a1.at[:, borrowed], y1_s, y1_r, yn).wait()

    def close(n, g_tile):
        v = c1[n] + dot(a1[:, k_rows(last_kg)], g_tile[...])
        v = v * v
        c1[n] = v
        s1[r, pl.ds(n, 1), :] = jnp.sum(v, axis=0, keepdims=True)

    def close_other(j):
        tile_copy(last_kg, j).wait()
        close(nh + j, gt.at[j])
    with scope("close"):
        unrolled(nh // 2, 2, lambda n: close(n, gown.at[n, k_rows(last_kg)]))
        unrolled(nf // 2, 2, close_other)
        for j in range(nf // 2 * 2, nf):
            close_other(j)
    for dev in (cn, xn, dn):
        remote(s1.at[r], s1.at[r], s1_s, s1_r, dev).start()
    with scope("wait_s1"):
        remote(a0.at[:, pl.ds(0, cols)], a0.at[:, pl.ds(0, cols)], ya_s, ya_r.at[0], yn).wait_send()
        three = s1.at[pl.ds(0, 3)]
        remote(three, three, s1_s, s1_r, cn).wait_recv()

    def rescale(n):
        line = pl.ds(n, 1)
        total = (s1[0, line, :] + s1[1, line, :]) + (s1[2, line, :] + s1[3, line, :])
        a0[:, chunk(n)] = (c1[n] * (n_all / total)).astype(BF16)
    with scope("rescale"):
        loop(nh - 1, nh + 1, rescale)
        remote(a0.at[:, lent], a2, y2_s, y2_r, yn).start()
        loop(0, nh - 1, rescale)
        loop(nh + 1, nc, rescale)

    near = nc * WIDTH

    def last(n):
        c1[n] = dot(a0[:, :near], gown[n, :near, :])
    with scope("last"):
        loop(0, nh, last)
    with scope("wait_a2"):
        remote(a0.at[:, lent], a2, y2_s, y2_r, yn).wait()

    def out_copy(n):
        return pltpu.make_async_copy(c1.at[n], out_ref.at[:, chunk(n)], out_sem.at[n])

    def end(n):
        v = c1[n] + dot(a2[...], gown[n, near:, :])
        v = v * v
        c1[n] = v
        s2[r, pl.ds(n, 1), :] = jnp.sum(v, axis=0, keepdims=True)
        out_copy(n).start()
    with scope("end"):
        loop(0, nh, end)

    for dev in (cn, xn, dn):
        remote(s2.at[r], s2.at[r], s2_s, s2_r, dev).start()

    def sent(ref, sem):
        remote(ref, ref, sem, s2_r, cn).wait_send()
    sent(gown.at[:, pl.ds(0, rows)], xown_s)
    sent(gown.at[pl.ds(0, nf), pl.ds(0, rows)], yg_s)
    sent(gown.at[:, pl.ds(0, rows)], cown_s)
    sent(gown.at[pl.ds(0, nf), pl.ds(0, rows)], xfwd_s)
    sent(gown.at[:, pl.ds(0, rows)], cfwd_s)
    sent(gown.at[pl.ds(0, nf), pl.ds(0, 2 * rows)], cfar_s)
    sent(sums.at[:, pl.ds(0, 3)], sum_s)
    sent(s1.at[pl.ds(0, 3)], s1_s)
    with scope("wait_s2"):
        three = s2.at[pl.ds(0, 3)]
        remote(three, three, s2_s, s2_r, cn).wait()
    total = (s2[0] + s2[1]) + (s2[2] + s2[3])
    for n in range(nh):
        sum_ref[:, n * WIDTH:(n + 1) * WIDTH] = total[n:n + 1]
    with scope("wait_out"):
        loop(0, nh, lambda n: out_copy(n).wait())


def scale_kernel(n_all, raw_ref, sum_ref, out_ref):
    out_ref[...] = raw_ref[...] * (n_all / sum_ref[...])


def solution(mesh):
    block_spec = P(("graph", "row"), "col")

    def device_step(init_blk, graph_blk):
        rows, cols = init_blk.shape
        n_all = 2 * cols
        nh = cols // WIDTH
        dma = pltpu.SemaphoreType.DMA
        any_spec = pl.BlockSpec(memory_space=pl.ANY)
        raw, col_sum, _ = pl.pallas_call(
            functools.partial(kernel, float(n_all)),
            out_shape=(
                jax.ShapeDtypeStruct((rows, cols), F32),
                jax.ShapeDtypeStruct((1, cols), F32),
                jax.ShapeDtypeStruct((nh - 1, n_all, WIDTH), BF16),
            ),
            in_specs=[any_spec, any_spec],
            out_specs=(any_spec, pl.BlockSpec(memory_space=pltpu.VMEM), any_spec),
            scratch_shapes=[
                pltpu.VMEM((rows, n_all), BF16),
                pltpu.VMEM((rows, n_all), BF16),
                pltpu.VMEM((rows, WIDTH), BF16),
                pltpu.VMEM((2 * nh, rows, WIDTH), F32),
                pltpu.VMEM((2, rows, WIDTH), F32),
                pltpu.VMEM((nh, n_all, WIDTH), BF16),
                pltpu.VMEM((2, n_all, WIDTH), BF16),
                pltpu.VMEM((nh - 1, 2 * WIDTH, WIDTH), BF16),
                pltpu.VMEM((2 * nh - 1, 4, 8, WIDTH), F32),
                pltpu.VMEM((4, 2 * nh, WIDTH), F32),
                pltpu.VMEM((4, nh, WIDTH), F32),
                dma((2 * nh,)), dma((2,)), dma((nh,)), dma((nh,)),
                dma((nh,)), dma((nh, PIECES)), dma((2,)), dma((nh, PIECES)), dma, dma,
                dma((2 * nh,)), dma((2 * nh,)), dma, dma,
                dma, dma, dma, dma, dma, dma, dma, dma, dma, dma, dma, dma,
            ],
            compiler_params=pltpu.CompilerParams(
                collective_id=0, has_side_effects=True, vmem_limit_bytes=62 * 2**20),
            name="mcl",
        )(init_blk, graph_blk)
        block = rows // 8
        line = pl.BlockSpec((block, cols), lambda i: (i, 0))
        return pl.pallas_call(
            functools.partial(scale_kernel, float(n_all)),
            out_shape=jax.ShapeDtypeStruct((rows, cols), F32),
            grid=(8,),
            in_specs=[line, pl.BlockSpec((1, cols), lambda i: (0, 0))],
            out_specs=line,
            name="scale",
        )(raw, col_sum)

    return jax.shard_map(device_step, mesh=mesh, in_specs=(block_spec, block_spec), out_specs=block_spec, check_vma=False)
```

```python
import contextlib
import functools

import jax
import jax.numpy as jnp
from jax import lax
from jax.experimental import pallas as pl
from jax.experimental.pallas import tpu as pltpu
from jax.sharding import PartitionSpec as P

MESH = pl.DeviceIdType.MESH
WIDTH = 256
PIECES = 8
TILE_M = 512
F32, BF16 = jnp.float32, jnp.bfloat16


def nothing(name):
    return contextlib.nullcontext()


scope = nothing


def dot(a, b):
    return jnp.dot(a, b, preferred_element_type=F32)


def kernel(n_all, flow_ref, graph_ref, out_ref, sum_ref, g_ref,
           a0, a1, a2, c1, mbuf, gown, gcol, gt, sums, s1, s2, parts,
           stage_sem, col_sem, gt_sem, out_sem,
           xown_r, xfwd_r, ya_r, yg_r, y1_r, y2_r, core_r, sum_r, s1_r, s2_r,
           xown_s, xfwd_s, ya_s, yg_s, y1_s, y2_s, cown_s, cfwd_s, cfar_s, sum_s, s1_s, s2_s):
    rows, cols = flow_ref.shape
    nh = cols // WIDTH
    nf = nh - 1
    nc = nh + nf
    depth = 4 * rows
    half = depth // 2
    quad = half // 2
    kg_rows = 2 * WIDTH
    prow = rows // PIECES

    y = lax.axis_index("col")
    r = lax.axis_index("row")
    z = lax.axis_index("graph")
    x = lax.div(r, 2)
    c = lax.rem(r, 2)
    xn = (z, y, (1 - x) * 2 + c)
    yn = (z, 1 - y, r)
    cn = (z, y, x * 2 + 1 - c)
    dn = (z, y, (1 - x) * 2 + 1 - c)
    lx = x + y - 2 * x * y
    own = pl.multiple_of((lx * 2 + c) * rows, rows)
    oth = pl.multiple_of(((1 - lx) * 2 + c) * rows, rows)
    mine, theirs = pl.ds(own, rows), pl.ds(oth, rows)

    def remote(src, dst, send, recv, dev):
        return pltpu.make_async_remote_copy(
            src_ref=src, dst_ref=dst, send_sem=send, recv_sem=recv, device_id=dev, device_id_type=MESH)

    def chunk(q):
        return pl.ds(pl.multiple_of(q * WIDTH, WIDTH), WIDTH)

    def stage_copy(k):
        src = graph_ref if k < nh else flow_ref
        return pltpu.make_async_copy(src.at[:, pl.ds((k % nh) * WIDTH, WIDTH)], c1.at[k], stage_sem.at[k])

    def stage(j):
        if j < nh:
            stage_copy(j).start()
            stage_copy(nh + j).start()

    stage(0)
    bar = pltpu.get_barrier_semaphore()
    for dev in (xn, yn, cn, dn):
        pl.semaphore_signal(bar, inc=1, device_id=dev, device_id_type=MESH)
    stage(1)
    stage(2)

    def send_own(j):
        block = gown.at[j, mine]
        remote(block, block, xown_s, xown_r.at[j], xn).start()
        piece = pl.ds(j * WIDTH, WIDTH)
        remote(a0.at[:, piece], a0.at[:, pl.ds(cols + j * WIDTH, WIDTH)], ya_s, ya_r.at[j * 2 // nh], yn).start()
        remote(block, block, cown_s, core_r.at[j], cn).start()

    for j in range(nh):
        with scope("cast"):
            stage_copy(j).wait()
            gown[j, mine, :] = c1[j].astype(BF16)
            stage_copy(nh + j).wait()
            a0[:, pl.ds(j * WIDTH, WIDTH)] = c1[nh + j].astype(BF16)
            stage(j + 3)
            if j == 1:
                with scope('barrier'):
                    pl.semaphore_wait(bar, 4)
            if j >= 1:
                send_own(j - 1)
    send_own(nh - 1)
    for j in range(nf):
        for p in range(PIECES):
            src = gown.at[j, pl.ds(own + p * prow, prow)]
            dst = g_ref.at[j, pl.ds(oth + p * prow, prow)]
            remote(src, dst, yg_s, yg_r.at[j, p], yn).start()

    n_pieces = nf * PIECES

    def relay(k, offset, sem, recv, dev, forward):
        @pl.when((k >= 0) & (k < n_pieces))
        def _():
            j, p = lax.div(k, PIECES), lax.rem(k, PIECES)
            piece = g_ref.at[j, pl.ds(pl.multiple_of(offset + p * prow, prow), prow)]
            remote(piece, piece, sem, recv.at[j, p], dev).wait_recv()
            if forward:
                remote(piece, piece, xfwd_s, xfwd_r.at[j, p], xn).start()
            remote(piece, piece, cfar_s, core_r.at[nh + j], cn).start()

    def relay_y(*ks):
        for k in ks:
            with scope("relay_y"):
                relay(jnp.int32(k), own, yg_s, yg_r, yn, True)

    def relayed(j):
        return PIECES * j + 13 + lax.max(0, 8 - 3 * j)

    def relay_x(*ks):
        for k in ks:
            with scope("relay_x"):
                relay(jnp.int32(k), oth, xfwd_s, xfwd_r, xn, False)

    lent, borrowed = pl.ds((nh - 1) * WIDTH, WIDTH), pl.ds((2 * nh - 1) * WIDTH, WIDTH)

    def wait_core(q):
        with scope("wait_core"):
            both = gown.at[0, pl.ds(0, half)]
            remote(both, both, cfwd_s, core_r.at[q], cn).wait_recv()

    def col_copy(q):
        slot = lax.rem(q, 2)
        return pltpu.make_async_copy(g_ref.at[q - nh], gcol.at[slot], col_sem.at[slot])

    def k_rows(kg):
        return pl.ds(pl.multiple_of(kg * kg_rows, kg_rows), kg_rows)

    def tile_copy(kg, j):
        return pltpu.make_async_copy(g_ref.at[j, k_rows(kg)], gt.at[j], gt_sem.at[j])

    def loop(lo, hi, body):
        def go(i, carry):
            body(i)
            return carry
        lax.fori_loop(lo, hi, go, 0)

    def over_m(body):
        loop(0, rows // TILE_M, lambda i: body(pl.ds(pl.multiple_of(i * TILE_M, TILE_M), TILE_M)))

    def fold(v):
        return jnp.sum(v.reshape(-1, 8, WIDTH), axis=0)

    def unrolled(n, width, body):
        def some(i):
            for t in range(width):
                body(i * width + t)
        loop(0, n, some)

    def first_half(q):
        wait_core(q)

        c1[q] = dot(a0[:, :cols], gown[q, :half, :])

    def third_quarter(q):
        c1[q] += dot(a0[:, cols:cols + quad], gown[q, half:half + quad, :])

    def wait_a(i):
        with scope("wait_a"):
            part = a0.at[:, pl.ds(0, quad)]
            remote(part, part, ya_s, ya_r.at[i], yn).wait_recv()

    def early(j):
        with scope("wait_xown"):
            block = gown.at[j, theirs]
            remote(block, block, xown_s, xown_r.at[j], xn).wait_recv()
        remote(block, block, cfwd_s, core_r.at[j], cn).start()

        @pl.when(j >= 1)
        def _():
            with scope("first_half"):
                first_half(j - 1)

        @pl.when(j == nh - 3)
        def _():
            wait_a(0)

        @pl.when(j >= nh - 3)
        def _():
            with scope("third_quarter"):
                first = 2 * (j - (nh - 3))
                third_quarter(first)
                third_quarter(first + 1)
    loop(0, nh, early)
    relay_y(0)
    with scope("early_end"):
        third_quarter(nh - 2)
        first_half(nh - 1)
        third_quarter(nh - 1)
    relay_y(1, 2)
    wait_a(1)

    def add_product(kg, n, g_tile):
        c1[n] += dot(a1[:, k_rows(kg)], g_tile[...])

    def finish(q, squares):
        with scope("finish"):
            three = sums.at[q, pl.ds(0, 3)]
            remote(three, three, sum_s, sum_r.at[q], cn).wait_recv()
            total = (sums[q, 0] + sums[q, 1]) + (sums[q, 2] + sums[q, 3])
            scale = n_all / jnp.sum(total, axis=0, keepdims=True)
            a1[:, chunk(q)] = (squares[...] * scale).astype(BF16)

    def send_sums(q):
        for dev in (cn, xn, dn):
            remote(sums.at[q, r], sums.at[q, r], sum_s, sum_r.at[q], dev).start()

    def own_expand(q):
        with scope("c0"):
            v = c1[q] + dot(a0[:, cols + quad:], gown[q, half + quad:, :])
            v = v * v
            c1[q] = v
            sums[q, r] = fold(v)
        send_sums(q)
        for at, k in ((0, 3), (2, 4), (3, 5), (5, 6), (7, 7)):
            @pl.when(q == at)
            def _():
                relay_y(k)
    loop(0, nh, own_expand)

    def own_finish(q):
        finish(q, c1.at[q])
        for at, k in ((2, 8), (3, 9), (5, 10), (7, 11)):
            @pl.when(q == at)
            def _():
                relay_y(k)
    loop(0, nh, own_finish)
    relay_x(0, 1, 2, 3, 4, 5, 6, 7)
    relay_y(12)
    remote(a1.at[:, lent], a1.at[:, borrowed], y1_s, y1_r, yn).start()

    def own_products(n):
        with scope("own_products"):
            c1[n] = dot(a1[:, :cols], gown[n, :half, :])
        relay_y(13 + n)

        @pl.when(n == 2)
        def _():
            wait_core(nh)
            col_copy(nh).start()
    loop(0, nh, own_products)

    def right_own(kg):
        def some(i):
            for n in range(4):
                c1[4 * i + n] += dot(a1[:, k_rows(kg)], gown[4 * i + n, k_rows(kg), :])
        with scope("right_own"):
            loop(0, nh // 4, some)

    def right_other(kg, pairs):
        def pair(i):
            for j in (2 * i, 2 * i + 1):
                tile_copy(kg, j).wait()
            for j in (2 * i, 2 * i + 1):
                c1[nh + j] += dot(a1[:, k_rows(kg)], gt[j])
        with scope("right_other"):
            loop(0, pairs, pair)

    def other_step(j):
        q = nh + j
        k = PIECES * j
        slot = lax.rem(q, 2)
        done = lax.div(q, 2)
        at_last = j == nf - 2
        paired = ((slot == 0) & (j > 0) & (j < nf - 1)) | at_last
        kg = lax.div(q - 1, 2)
        pairs = lax.div(j + 1, 2)
        ahead = relayed(j)

        def relay_ahead(*steps):
            for i in steps:
                @pl.when(ahead + i < relayed(j + 1))
                def _():
                    relay_y(ahead + i)

        def relay_next(*steps):
            for i in steps:
                relay_x(k + PIECES + i)
        with scope("load"):
            col_copy(q).wait()

        @pl.when(paired)
        def _():
            loop(0, 2 * pairs, lambda i: tile_copy(kg, i).start())
        relay_ahead(0)
        sums[q, r] = jnp.zeros((8, WIDTH), F32)

        def expand(m):
            v = dot(a0[m, :], gcol[slot])
            v = v * v
            mbuf[slot, m, :] = v
            sums[q, r] += fold(v)
        with scope("c0"):
            over_m(expand)
        send_sums(q)
        relay_ahead(1, 2)
        relay_next(0, 1, 2)

        @pl.when((j > 0) & (j < nf - 1))
        def _():
            finish(q - 1, mbuf.at[1 - slot])

        def expand_flow(m):
            c1[q, m, :] = dot(a1[m, :cols], gcol[slot, :half, :])
        with scope("left"):
            over_m(expand_flow)
            loop(nh // 2, done, lambda i: add_product(i, q, gcol.at[slot, k_rows(i)]))
        relay_ahead(3)
        relay_next(3, 4)

        @pl.when(at_last)
        def _():
            finish(q, mbuf.at[slot])

        @pl.when(paired)
        def _():
            right_own(kg)
        relay_next(5)
        relay_ahead(4)
        relay_next(6)
        relay_ahead(5)
        relay_next(7)

        @pl.when(j + 1 < nf)
        def _():
            wait_core(q + 1)
            col_copy(q + 1).start()

        @pl.when(paired)
        def _():
            right_other(kg, pairs)
        relay_ahead(6, 7)
    loop(0, nf, other_step)

    last_kg = nh - 1
    loop(0, nf, lambda j: tile_copy(last_kg, j).start())
    parts[2 * nh - 1] = jnp.zeros((8, WIDTH), F32)
    finish(nc - 1, mbuf.at[(nc - 1) % 2])
    with scope("wait_a1"):
        remote(a1.at[:, lent], a1.at[:, borrowed], y1_s, y1_r, yn).wait()

    def close(n, g_tile):
        v = c1[n] + dot(a1[:, k_rows(last_kg)], g_tile[...])
        v = v * v
        c1[n] = v
        parts[n] = fold(v)

    def close_other(j):
        tile_copy(last_kg, j).wait()
        close(nh + j, gt.at[j])
    def send_s1(i):
        part = s1.at[i, r]
        for dev in (cn, xn, dn):
            remote(part, part, s1_s, s1_r.at[i], dev).start()

    with scope("close"):
        unrolled(nh // 4, 4, lambda n: close(n, gown.at[n, k_rows(last_kg)]))
        s1[0, r] = jnp.sum(parts[:nh], axis=1)
    send_s1(0)
    with scope("close"):
        unrolled(nf // 2, 2, close_other)
        for j in range(nf // 2 * 2, nf):
            close_other(j)
        s1[1, r] = jnp.sum(parts[nh:], axis=1)
    send_s1(1)

    def wait_s1(i):
        with scope("wait_s1"):
            three = s1.at[i, pl.ds(0, 3)]
            remote(three, three, s1_s, s1_r.at[i], cn).wait_recv()

    def rescale(i, n):
        line = pl.ds(n, 1)
        total = (s1[i, 0, line, :] + s1[i, 1, line, :]) + (s1[i, 2, line, :] + s1[i, 3, line, :])
        a0[:, chunk(i * nh + n)] = (c1[i * nh + n] * (n_all / total)).astype(BF16)

    remote(a0.at[:, pl.ds(0, cols)], a0.at[:, pl.ds(0, cols)], ya_s, ya_r.at[0], yn).wait_send()
    wait_s1(0)
    with scope("rescale"):
        loop(0, nh, lambda i: rescale(0, nh - 1 - i))

    near = nc * WIDTH

    def out_copy(n):
        return pltpu.make_async_copy(c1.at[n], out_ref.at[:, chunk(n)], out_sem.at[n])

    def put(n, v):
        v = v * v
        c1[n] = v
        parts[n] = fold(v)

    def last_near(n):
        c1[n] = dot(a0[:, :cols], gown[n, :half, :])

    def last_other(n):
        c1[n] += dot(a0[:, cols:near], gown[n, half:near, :])

    def last(n):
        c1[n] = dot(a0[:, :near], gown[n, :near, :])

    def last_far(i):
        put(2 * i, c1[2 * i] + dot(a2[...], gown[2 * i, near:, :]))
        put(2 * i + 1, c1[2 * i + 1] + dot(a2[...], gown[2 * i + 1, near:, :]))
        out_copy(2 * i).start()
        out_copy(2 * i + 1).start()

    def last_whole(n):
        put(n, dot(a0[:, :near], gown[n, :near, :]) + dot(a2[...], gown[n, near:, :]))
        out_copy(n).start()
    with scope("last_near"):
        remote(a0.at[:, lent], a2, y2_s, y2_r, yn).start()
        loop(0, 2, last_near)
    wait_s1(1)
    with scope("rescale"):
        loop(0, nf, lambda n: rescale(1, n))
    with scope("last"):
        loop(0, 2, last_other)
        loop(2, nh - 2, last)
    with scope("wait_a2"):
        remote(a0.at[:, lent], a2, y2_s, y2_r, yn).wait()
    with scope("last_far"):
        loop(0, (nh - 2) // 2, last_far)
    with scope("last_whole"):
        loop(nh - 2, nh, last_whole)
        s2[r] = jnp.sum(parts[:nh], axis=1)

    for dev in (cn, xn, dn):
        remote(s2.at[r], s2.at[r], s2_s, s2_r, dev).start()

    def sent(ref, sem):
        remote(ref, ref, sem, s2_r, cn).wait_send()
    sent(gown.at[:, pl.ds(0, rows)], xown_s)
    sent(gown.at[pl.ds(0, nf), pl.ds(0, rows)], yg_s)
    sent(gown.at[:, pl.ds(0, rows)], cown_s)
    sent(gown.at[pl.ds(0, nf), pl.ds(0, rows)], xfwd_s)
    sent(gown.at[:, pl.ds(0, rows)], cfwd_s)
    sent(gown.at[pl.ds(0, nf), pl.ds(0, 2 * rows)], cfar_s)
    sent(sums.at[:, pl.ds(0, 3)], sum_s)
    sent(s1.at[:, pl.ds(0, 3)], s1_s)
    with scope("wait_s2"):
        three = s2.at[pl.ds(0, 3)]
        remote(three, three, s2_s, s2_r, cn).wait()
    total = (s2[0] + s2[1]) + (s2[2] + s2[3])
    for n in range(nh):
        sum_ref[:, n * WIDTH:(n + 1) * WIDTH] = total[n:n + 1]
    with scope("wait_out"):
        loop(0, nh, lambda n: out_copy(n).wait())


BLOCKS = 8


def scale_kernel(n_all, raw_ref, sum_ref, out_ref, buf, in_sem, out_sem):
    rows = buf.shape[1]

    def get(i):
        return pltpu.make_async_copy(raw_ref.at[pl.ds(i * rows, rows)], buf.at[i], in_sem.at[i])

    def put(i):
        return pltpu.make_async_copy(buf.at[i], out_ref.at[pl.ds(i * rows, rows)], out_sem.at[i])

    for i in range(BLOCKS):
        get(i).start()
    scale = n_all / sum_ref[...]
    for i in range(BLOCKS):
        get(i).wait()
        buf[i] = buf[i] * scale
        put(i).start()
    for i in range(BLOCKS):
        put(i).wait()


def solution(mesh):
    block_spec = P(("graph", "row"), "col")

    def device_step(init_blk, graph_blk):
        rows, cols = init_blk.shape
        n_all = 2 * cols
        nh = cols // WIDTH
        dma = pltpu.SemaphoreType.DMA
        any_spec = pl.BlockSpec(memory_space=pl.ANY)
        raw, col_sum, _ = pl.pallas_call(
            functools.partial(kernel, float(n_all)),
            out_shape=(
                jax.ShapeDtypeStruct((rows, cols), F32),
                jax.ShapeDtypeStruct((1, cols), F32),
                jax.ShapeDtypeStruct((nh - 1, n_all, WIDTH), BF16),
            ),
            in_specs=[any_spec, any_spec],
            out_specs=(any_spec, pl.BlockSpec(memory_space=pltpu.VMEM), any_spec),
            scratch_shapes=[
                pltpu.VMEM((rows, n_all), BF16),
                pltpu.VMEM((rows, n_all), BF16),
                pltpu.VMEM((rows, WIDTH), BF16),
                pltpu.VMEM((2 * nh, rows, WIDTH), F32),
                pltpu.VMEM((2, rows, WIDTH), F32),
                pltpu.VMEM((nh, n_all, WIDTH), BF16),
                pltpu.VMEM((2, n_all, WIDTH), BF16),
                pltpu.VMEM((nh - 1, 2 * WIDTH, WIDTH), BF16),
                pltpu.VMEM((2 * nh - 1, 4, 8, WIDTH), F32),
                pltpu.VMEM((2, 4, nh, WIDTH), F32),
                pltpu.VMEM((4, nh, WIDTH), F32),
                pltpu.VMEM((2 * nh, 8, WIDTH), F32),
                dma((2 * nh,)), dma((2,)), dma((nh,)), dma((nh,)),
                dma((nh,)), dma((nh, PIECES)), dma((2,)), dma((nh, PIECES)), dma, dma,
                dma((2 * nh,)), dma((2 * nh,)), dma((2,)), dma,
                dma, dma, dma, dma, dma, dma, dma, dma, dma, dma, dma, dma,
            ],
            compiler_params=pltpu.CompilerParams(
                collective_id=0, has_side_effects=True, vmem_limit_bytes=62 * 2**20),
            name="mcl",
        )(init_blk, graph_blk)
        dma_blocks = dma((BLOCKS,))
        return pl.pallas_call(
            functools.partial(scale_kernel, float(n_all)),
            out_shape=jax.ShapeDtypeStruct((rows, cols), F32),
            in_specs=[any_spec, pl.BlockSpec(memory_space=pltpu.VMEM)],
            out_specs=any_spec,
            scratch_shapes=[pltpu.VMEM((BLOCKS, rows // BLOCKS, cols), F32), dma_blocks, dma_blocks],
            compiler_params=pltpu.CompilerParams(vmem_limit_bytes=62 * 2**20),
            name="scale",
        )(raw, col_sum)

    return jax.shard_map(device_step, mesh=mesh, in_specs=(block_spec, block_spec), out_specs=block_spec, check_vma=False)
```

```python
import contextlib
import functools

import jax
import jax.numpy as jnp
from jax import lax
from jax.experimental import pallas as pl
from jax.experimental.pallas import tpu as pltpu
from jax.sharding import PartitionSpec as P

MESH = pl.DeviceIdType.MESH
WIDTH = 256
PIECES = 8
TILE_M = 512
F32, BF16 = jnp.float32, jnp.bfloat16


def nothing(name):
    return contextlib.nullcontext()


scope = nothing


def dot(a, b):
    return jnp.dot(a, b, preferred_element_type=F32)


def kernel(n_all, flow_ref, graph_ref, c1, sum_ref, g_ref,
           a0, a1, a2, c1o, mbuf, gown, gcol, gt, sums, s1, s2, parts,
           stage_sem, col_sem, gt_sem,
           xown_r, xfwd_r, ya_r, yg_r, y1_r, y2_r, core_r, sum_r, s1_r, s2_r,
           xown_s, xfwd_s, ya_s, yg_s, y1_s, y2_s, cown_s, cfwd_s, cfar_s, sum_s, s1_s, s2_s):
    rows, cols = flow_ref.shape
    nh = cols // WIDTH
    nf = nh - 1
    nc = nh + nf
    depth = 4 * rows
    half = depth // 2
    quad = half // 2
    kg_rows = 2 * WIDTH
    prow = rows // PIECES

    y = lax.axis_index("col")
    r = lax.axis_index("row")
    z = lax.axis_index("graph")
    x = lax.div(r, 2)
    c = lax.rem(r, 2)
    xn = (z, y, (1 - x) * 2 + c)
    yn = (z, 1 - y, r)
    cn = (z, y, x * 2 + 1 - c)
    dn = (z, y, (1 - x) * 2 + 1 - c)
    lx = x + y - 2 * x * y
    own = pl.multiple_of((lx * 2 + c) * rows, rows)
    oth = pl.multiple_of(((1 - lx) * 2 + c) * rows, rows)
    mine, theirs = pl.ds(own, rows), pl.ds(oth, rows)

    def remote(src, dst, send, recv, dev):
        return pltpu.make_async_remote_copy(
            src_ref=src, dst_ref=dst, send_sem=send, recv_sem=recv, device_id=dev, device_id_type=MESH)

    def chunk(q):
        return pl.ds(pl.multiple_of(q * WIDTH, WIDTH), WIDTH)

    def stage_copy(k):
        src = graph_ref if k < nh else flow_ref
        return pltpu.make_async_copy(src.at[:, pl.ds((k % nh) * WIDTH, WIDTH)],
                                     c1.at[k] if k < nh else c1o.at[k - nh], stage_sem.at[k])

    def stage(j):
        if j < nh:
            stage_copy(j).start()
            stage_copy(nh + j).start()

    gt[nh - 1] = jnp.zeros((kg_rows, WIDTH), BF16)
    stage(0)
    bar = pltpu.get_barrier_semaphore()
    for dev in (xn, yn, cn, dn):
        pl.semaphore_signal(bar, inc=1, device_id=dev, device_id_type=MESH)
    stage(1)
    stage(2)

    def send_own(j):
        block = gown.at[j, mine]
        remote(block, block, xown_s, xown_r.at[j], xn).start()
        piece = pl.ds(j * WIDTH, WIDTH)
        remote(a0.at[:, piece], a0.at[:, pl.ds(cols + j * WIDTH, WIDTH)], ya_s, ya_r.at[j * 2 // nh], yn).start()
        remote(block, block, cown_s, core_r.at[j], cn).start()

    for j in range(nh):
        with scope("cast"):
            stage_copy(j).wait()
            gown[j, mine, :] = c1[j].astype(BF16)
            stage_copy(nh + j).wait()
            a0[:, pl.ds(j * WIDTH, WIDTH)] = c1o[j].astype(BF16)
            stage(j + 3)
            if j == 1:
                with scope('barrier'):
                    pl.semaphore_wait(bar, 4)
            if j >= 1:
                send_own(j - 1)
    send_own(nh - 1)
    for j in range(nf):
        for p in range(PIECES):
            src = gown.at[j, pl.ds(own + p * prow, prow)]
            dst = g_ref.at[j, pl.ds(oth + p * prow, prow)]
            remote(src, dst, yg_s, yg_r.at[j, p], yn).start()

    n_pieces = nf * PIECES

    def relay(k, offset, sem, recv, dev, forward):
        @pl.when((k >= 0) & (k < n_pieces))
        def _():
            j, p = lax.div(k, PIECES), lax.rem(k, PIECES)
            piece = g_ref.at[j, pl.ds(pl.multiple_of(offset + p * prow, prow), prow)]
            remote(piece, piece, sem, recv.at[j, p], dev).wait_recv()
            if forward:
                remote(piece, piece, xfwd_s, xfwd_r.at[j, p], xn).start()
            remote(piece, piece, cfar_s, core_r.at[nh + j], cn).start()

    def relay_y(*ks):
        for k in ks:
            with scope("relay_y"):
                relay(jnp.int32(k), own, yg_s, yg_r, yn, True)

    def relayed(j):
        return PIECES * j + 13 + lax.max(0, 6 - 4 * j)

    def relay_x(*ks):
        for k in ks:
            with scope("relay_x"):
                relay(jnp.int32(k), oth, xfwd_s, xfwd_r, xn, False)

    lent, borrowed = pl.ds((nh - 1) * WIDTH, WIDTH), pl.ds((2 * nh - 1) * WIDTH, WIDTH)

    def wait_core(q):
        with scope("wait_core"):
            both = gown.at[0, pl.ds(0, half)]
            remote(both, both, cfwd_s, core_r.at[q], cn).wait_recv()

    def col_copy(q):
        slot = lax.rem(q, 2)
        return pltpu.make_async_copy(g_ref.at[q - nh], gcol.at[slot], col_sem.at[slot])

    def k_rows(kg):
        return pl.ds(pl.multiple_of(kg * kg_rows, kg_rows), kg_rows)

    def tile_copy(kg, j):
        return pltpu.make_async_copy(g_ref.at[j, k_rows(kg)], gt.at[j], gt_sem.at[j])

    def loop(lo, hi, body):
        def go(i, carry):
            body(i)
            return carry
        lax.fori_loop(lo, hi, go, 0)

    def over_m(body):
        loop(0, rows // TILE_M, lambda i: body(pl.ds(pl.multiple_of(i * TILE_M, TILE_M), TILE_M)))

    def fold(v):
        return jnp.sum(v.reshape(-1, 8, WIDTH), axis=0)

    def unrolled(n, width, body):
        def some(i):
            for t in range(width):
                body(i * width + t)
        loop(0, n, some)

    def first_half(q):
        wait_core(q)

        c1[q] = dot(a0[:, :cols], gown[q, :half, :])

    def third_quarter(q):
        c1[q] += dot(a0[:, cols:cols + quad], gown[q, half:half + quad, :])

    def wait_a(i):
        with scope("wait_a"):
            part = a0.at[:, pl.ds(0, quad)]
            remote(part, part, ya_s, ya_r.at[i], yn).wait_recv()

    def early(j):
        with scope("wait_xown"):
            block = gown.at[j, theirs]
            remote(block, block, xown_s, xown_r.at[j], xn).wait_recv()
        remote(block, block, cfwd_s, core_r.at[j], cn).start()

        @pl.when(j >= 1)
        def _():
            with scope("first_half"):
                first_half(j - 1)

        @pl.when(j == nh - 3)
        def _():
            wait_a(0)

        @pl.when(j >= nh - 3)
        def _():
            with scope("third_quarter"):
                first = 2 * (j - (nh - 3))
                third_quarter(first)
                third_quarter(first + 1)
    loop(0, nh, early)
    relay_y(0)
    with scope("early_end"):
        third_quarter(nh - 2)
        first_half(nh - 1)
        third_quarter(nh - 1)
    relay_y(1, 2)
    wait_a(1)

    def add_other(kg, j, g_tile):
        c1o[j] += dot(a1[:, k_rows(kg)], g_tile[...])

    def finish(q, squares):
        with scope("finish"):
            three = sums.at[q, pl.ds(0, 3)]
            remote(three, three, sum_s, sum_r.at[q], cn).wait_recv()
            total = (sums[q, 0] + sums[q, 1]) + (sums[q, 2] + sums[q, 3])
            scale = n_all / jnp.sum(total, axis=0, keepdims=True)
            a1[:, chunk(q)] = (squares[...] * scale).astype(BF16)

    def send_sums(q):
        for dev in (cn, xn, dn):
            remote(sums.at[q, r], sums.at[q, r], sum_s, sum_r.at[q], dev).start()

    def own_expand(q):
        with scope("c0"):
            v = c1[q] + dot(a0[:, cols + quad:], gown[q, half + quad:, :])
            v = v * v
            c1[q] = v
            sums[q, r] = fold(v)
        send_sums(q)
        for at, k in ((0, 3), (2, 4), (3, 5), (5, 6), (7, 7)):
            @pl.when(q == at)
            def _():
                relay_y(k)
    loop(0, nh, own_expand)

    def after(i, *relays):
        for at, k in relays:
            @pl.when(i == at)
            def _():
                relay_y(k)

    def own_finish(q):
        finish(q, c1.at[q])
        after(q, (1, 8), (3, 9), (7, 12))

    def own_first(n):
        with scope("own_first"):
            c1[n] = dot(a1[:, :quad], gown[n, :quad, :])
        after(n, (0, 10), (2, 11))

    def own_second(n):
        with scope("own_second"):
            c1[n] += dot(a1[:, quad:cols], gown[n, quad:half, :])
        after(n, (1, 13), (3, 14))

    def own_whole(n):
        with scope("own_whole"):
            c1[n] = dot(a1[:, :cols], gown[n, :half, :])
        relay_y(15 - nh // 2 + n)
    loop(0, nh // 2, own_finish)
    loop(0, nh // 2, own_first)
    loop(nh // 2, nh, own_finish)
    relay_x(0, 1, 2, 3, 4, 5, 6, 7)
    loop(0, nh // 2, own_second)
    remote(a1.at[:, lent], a1.at[:, borrowed], y1_s, y1_r, yn).start()
    wait_core(nh)
    col_copy(nh).start()
    loop(nh // 2, nh, own_whole)

    def right_own(kg):
        def some(i):
            for n in range(4):
                c1[4 * i + n] += dot(a1[:, k_rows(kg)], gown[4 * i + n, k_rows(kg), :])
        with scope("right_own"):
            loop(0, nh // 4, some)

    def right_one(q):
        k_one = chunk(q)

        def some(i):
            for n in range(4):
                c1[4 * i + n] += dot(a1[:, k_one], gown[4 * i + n, k_one, :])
        with scope("right_one"):
            loop(0, nh // 4, some)

    def right_other(kg, pairs):
        def pair(i):
            for j in (2 * i, 2 * i + 1):
                tile_copy(kg, j).wait()
            for j in (2 * i, 2 * i + 1):
                add_other(kg, j, gt.at[j])
        with scope("right_other"):
            loop(0, pairs, pair)

    def other_step(j):
        q = nh + j
        k = PIECES * j
        slot = lax.rem(q, 2)
        done = lax.div(q, 2)
        at_last = j == nf - 2
        paired = ((slot == 0) & (j > 0) & (j < nf - 1)) | at_last
        kg = lax.div(q - 1, 2)
        pairs = lax.div(j + 1, 2)
        ahead = relayed(j)

        def relay_ahead(*steps):
            for i in steps:
                @pl.when(ahead + i < relayed(j + 1))
                def _():
                    relay_y(ahead + i)

        def relay_next(*steps):
            for i in steps:
                relay_x(k + PIECES + i)
        with scope("load"):
            col_copy(q).wait()

        @pl.when(paired)
        def _():
            loop(0, 2 * pairs, lambda i: tile_copy(kg, i).start())
        relay_ahead(0)
        sums[q, r] = jnp.zeros((8, WIDTH), F32)

        def expand(m):
            v = dot(a0[m, :], gcol[slot])
            v = v * v
            mbuf[slot, m, :] = v
            sums[q, r] += fold(v)
        with scope("c0"):
            over_m(expand)
        send_sums(q)
        relay_ahead(1, 2)
        relay_next(0, 1, 2)

        @pl.when((j > 0) & (j < nf - 1))
        def _():
            finish(q - 1, mbuf.at[1 - slot])

        def expand_flow(m):
            c1o[j, m, :] = dot(a1[m, :cols], gcol[slot, :half, :])
        with scope("left"):
            over_m(expand_flow)
            loop(nh // 2, done, lambda i: add_other(i, j, gcol.at[slot, k_rows(i)]))
        relay_ahead(3)
        relay_next(3, 4)

        @pl.when(at_last)
        def _():
            right_one(q - 1)
            finish(q, mbuf.at[slot])
            right_one(q)

        @pl.when(paired & ~at_last)
        def _():
            right_own(kg)
        relay_next(5)
        relay_ahead(4)
        relay_next(6)
        relay_ahead(5)
        relay_next(7)

        @pl.when(j + 1 < nf)
        def _():
            wait_core(q + 1)
            col_copy(q + 1).start()

        @pl.when(paired)
        def _():
            right_other(kg, pairs)
        relay_ahead(6, 7)
    loop(0, nf, other_step)

    last_kg = nh - 1
    loop(0, nf, lambda j: tile_copy(last_kg, j).start())
    finish(nc - 1, mbuf.at[(nc - 1) % 2])
    with scope("wait_a1"):
        remote(a1.at[:, lent], a1.at[:, borrowed], y1_s, y1_r, yn).wait()

    def close(c, i, part, g_tile):
        v = c[i] + dot(a1[:, k_rows(last_kg)], g_tile[...])
        v = v * v
        c[i] = v
        parts[part] = fold(v)

    def close_other(j):
        close(c1o, j, nh + j, gt.at[j])

    def send_s1(i):
        part = s1.at[i, r]
        for dev in (cn, xn, dn):
            remote(part, part, s1_s, s1_r.at[i], dev).start()

    with scope("close"):
        unrolled(nh // 4, 4, lambda n: close(c1, n, n, gown.at[n, k_rows(last_kg)]))
        s1[0, r] = jnp.sum(parts[:nh], axis=1)
    send_s1(0)
    with scope("close"):
        loop(0, nf, lambda j: tile_copy(last_kg, j).wait())
        unrolled(nh // 4, 4, close_other)
        s1[1, r] = jnp.sum(parts[nh:], axis=1)
    send_s1(1)

    def wait_s1(i):
        with scope("wait_s1"):
            three = s1.at[i, pl.ds(0, 3)]
            remote(three, three, s1_s, s1_r.at[i], cn).wait_recv()

    def rescale(i, n):
        line = pl.ds(n, 1)
        total = (s1[i, 0, line, :] + s1[i, 1, line, :]) + (s1[i, 2, line, :] + s1[i, 3, line, :])
        a0[:, chunk(i * nh + n)] = ((c1 if i == 0 else c1o)[n] * (n_all / total)).astype(BF16)

    remote(a0.at[:, pl.ds(0, cols)], a0.at[:, pl.ds(0, cols)], ya_s, ya_r.at[0], yn).wait_send()
    wait_s1(0)
    with scope("rescale"):
        loop(0, nh, lambda i: rescale(0, nh - 1 - i))

    near = nc * WIDTH

    def put(n, v):
        v = v * v
        c1[n] = v
        parts[n] = fold(v)

    def last_near(n):
        c1[n] = dot(a0[:, :cols], gown[n, :half, :])

    def last_other(n):
        c1[n] += dot(a0[:, cols:near], gown[n, half:near, :])

    def last(n):
        c1[n] = dot(a0[:, :near], gown[n, :near, :])

    def last_far(i):
        put(2 * i, c1[2 * i] + dot(a2[...], gown[2 * i, near:, :]))
        put(2 * i + 1, c1[2 * i + 1] + dot(a2[...], gown[2 * i + 1, near:, :]))

    def last_whole(n):
        put(n, dot(a0[:, :near], gown[n, :near, :]) + dot(a2[...], gown[n, near:, :]))
    with scope("last_near"):
        remote(a0.at[:, lent], a2, y2_s, y2_r, yn).start()
        loop(0, 2, last_near)
    wait_s1(1)
    with scope("rescale"):
        loop(0, nf, lambda n: rescale(1, n))
    with scope("last"):
        loop(0, 2, last_other)
        loop(2, nh - 2, last)
    with scope("wait_a2"):
        remote(a0.at[:, lent], a2, y2_s, y2_r, yn).wait()
    with scope("last_far"):
        loop(0, (nh - 2) // 2, last_far)
    with scope("last_whole"):
        loop(nh - 2, nh, last_whole)
        s2[r] = jnp.sum(parts[:nh], axis=1)

    for dev in (cn, xn, dn):
        remote(s2.at[r], s2.at[r], s2_s, s2_r, dev).start()

    def sent(ref, sem):
        remote(ref, ref, sem, s2_r, cn).wait_send()
    sent(gown.at[:, pl.ds(0, rows)], xown_s)
    sent(gown.at[pl.ds(0, nf), pl.ds(0, rows)], yg_s)
    sent(gown.at[:, pl.ds(0, rows)], cown_s)
    sent(gown.at[pl.ds(0, nf), pl.ds(0, rows)], xfwd_s)
    sent(gown.at[:, pl.ds(0, rows)], cfwd_s)
    sent(gown.at[pl.ds(0, nf), pl.ds(0, 2 * rows)], cfar_s)
    sent(sums.at[:, pl.ds(0, 3)], sum_s)
    sent(s1.at[:, pl.ds(0, 3)], s1_s)
    with scope("wait_s2"):
        three = s2.at[pl.ds(0, 3)]
        remote(three, three, s2_s, s2_r, cn).wait()
    total = (s2[0] + s2[1]) + (s2[2] + s2[3])
    for n in range(nh):
        sum_ref[:, n * WIDTH:(n + 1) * WIDTH] = total[n:n + 1]


def scale_kernel(n_all, raw_ref, sum_ref, out_ref, buf, out_sem):
    def put(i):
        return pltpu.make_async_copy(buf.at[i], out_ref.at[:, pl.ds(i * WIDTH, WIDTH)], out_sem.at[i])

    chunks = raw_ref.shape[0]
    for i in range(chunks):
        buf[i] = raw_ref[i] * (n_all / sum_ref[:, i * WIDTH:(i + 1) * WIDTH])
        put(i).start()
    for i in range(chunks):
        put(i).wait()


def solution(mesh):
    block_spec = P(("graph", "row"), "col")

    def device_step(init_blk, graph_blk):
        rows, cols = init_blk.shape
        n_all = 2 * cols
        nh = cols // WIDTH
        dma = pltpu.SemaphoreType.DMA
        any_spec, vmem_spec = pl.BlockSpec(memory_space=pl.ANY), pl.BlockSpec(memory_space=pltpu.VMEM)
        raw, col_sum, _ = pl.pallas_call(
            functools.partial(kernel, float(n_all)),
            out_shape=(
                pltpu.VMEM((nh, rows, WIDTH), F32),
                pltpu.VMEM((1, cols), F32),
                jax.ShapeDtypeStruct((nh - 1, n_all, WIDTH), BF16),
            ),
            in_specs=[any_spec, any_spec],
            out_specs=(vmem_spec, vmem_spec, any_spec),
            scratch_shapes=[
                pltpu.VMEM((rows, n_all), BF16),
                pltpu.VMEM((rows, n_all), BF16),
                pltpu.VMEM((rows, WIDTH), BF16),
                pltpu.VMEM((nh, rows, WIDTH), F32),
                pltpu.VMEM((2, rows, WIDTH), F32),
                pltpu.VMEM((nh, n_all, WIDTH), BF16),
                pltpu.VMEM((2, n_all, WIDTH), BF16),
                pltpu.VMEM((nh, 2 * WIDTH, WIDTH), BF16),
                pltpu.VMEM((2 * nh - 1, 4, 8, WIDTH), F32),
                pltpu.VMEM((2, 4, nh, WIDTH), F32),
                pltpu.VMEM((4, nh, WIDTH), F32),
                pltpu.VMEM((2 * nh, 8, WIDTH), F32),
                dma((2 * nh,)), dma((2,)), dma((nh,)),
                dma((nh,)), dma((nh, PIECES)), dma((2,)), dma((nh, PIECES)), dma, dma,
                dma((2 * nh,)), dma((2 * nh,)), dma((2,)), dma,
                dma, dma, dma, dma, dma, dma, dma, dma, dma, dma, dma, dma,
            ],
            compiler_params=pltpu.CompilerParams(
                collective_id=0, has_side_effects=True, vmem_limit_bytes=54 * 2**20),
            name="mcl",
        )(init_blk, graph_blk)
        return pl.pallas_call(
            functools.partial(scale_kernel, float(n_all)),
            out_shape=jax.ShapeDtypeStruct((rows, cols), F32),
            in_specs=[vmem_spec, vmem_spec],
            out_specs=any_spec,
            scratch_shapes=[pltpu.VMEM((nh, rows, WIDTH), F32), dma((nh,))],
            compiler_params=pltpu.CompilerParams(vmem_limit_bytes=40 * 2**20),
            name="scale",
        )(raw, col_sum)

    return jax.shard_map(device_step, mesh=mesh, in_specs=(block_spec, block_spec), out_specs=block_spec, check_vma=False)
```

```python
import contextlib
import functools

import jax
import jax.numpy as jnp
from jax import lax
from jax.experimental import pallas as pl
from jax.experimental.pallas import tpu as pltpu
from jax.sharding import PartitionSpec as P

MESH = pl.DeviceIdType.MESH
WIDTH = 256
PIECES = 8
TILE_M = 512
F32, BF16 = jnp.float32, jnp.bfloat16


def nothing(name):
    return contextlib.nullcontext()


scope = nothing


def dot(a, b):
    return jnp.dot(a, b, preferred_element_type=F32)


def kernel(n_all, flow_ref, graph_ref, c1, sum_ref, g_ref,
           a0, a1, a2, c1o, mbuf, gown, gcol, gt, sums, s1, s2, parts,
           stage_sem, col_sem, gt_sem,
           xown_r, xfwd_r, ya_r, yg_r, y1_r, y2_r, core_r, sum_r, s1_r, s2_r,
           xown_s, xfwd_s, ya_s, yg_s, y1_s, y2_s, cown_s, cfwd_s, cfar_s, sum_s, s1_s, s2_s):
    rows, cols = flow_ref.shape
    nh = cols // WIDTH
    nf = nh - 1
    nc = nh + nf
    depth = 4 * rows
    half = depth // 2
    quad = half // 2
    kg_rows = 2 * WIDTH
    prow = rows // PIECES

    y = lax.axis_index("col")
    r = lax.axis_index("row")
    z = lax.axis_index("graph")
    x = lax.div(r, 2)
    c = lax.rem(r, 2)
    xn = (z, y, (1 - x) * 2 + c)
    yn = (z, 1 - y, r)
    cn = (z, y, x * 2 + 1 - c)
    dn = (z, y, (1 - x) * 2 + 1 - c)
    lx = x + y - 2 * x * y
    own = pl.multiple_of((lx * 2 + c) * rows, rows)
    oth = pl.multiple_of(((1 - lx) * 2 + c) * rows, rows)
    mine, theirs = pl.ds(own, rows), pl.ds(oth, rows)

    def remote(src, dst, send, recv, dev):
        return pltpu.make_async_remote_copy(
            src_ref=src, dst_ref=dst, send_sem=send, recv_sem=recv, device_id=dev, device_id_type=MESH)

    def chunk(q):
        return pl.ds(pl.multiple_of(q * WIDTH, WIDTH), WIDTH)

    def stage_copy(k):
        src = graph_ref if k < nh else flow_ref
        return pltpu.make_async_copy(src.at[:, pl.ds((k % nh) * WIDTH, WIDTH)],
                                     c1.at[k] if k < nh else c1o.at[k - nh], stage_sem.at[k])

    def stage(j):
        if j < nh:
            stage_copy(j).start()
            stage_copy(nh + j).start()

    gt[nh - 1] = jnp.zeros((kg_rows, WIDTH), BF16)
    stage(0)
    bar = pltpu.get_barrier_semaphore()
    for dev in (xn, yn, cn, dn):
        pl.semaphore_signal(bar, inc=1, device_id=dev, device_id_type=MESH)
    stage(1)
    stage(2)

    def send_own(j):
        block = gown.at[j, mine]
        remote(block, block, xown_s, xown_r.at[j], xn).start()
        piece = pl.ds(j * WIDTH, WIDTH)
        remote(a0.at[:, piece], a0.at[:, pl.ds(cols + j * WIDTH, WIDTH)], ya_s, ya_r.at[j * 2 // nh], yn).start()
        remote(block, block, cown_s, core_r.at[j], cn).start()

    for j in range(nh):
        with scope("cast"):
            stage_copy(j).wait()
            gown[j, mine, :] = c1[j].astype(BF16)
            stage_copy(nh + j).wait()
            a0[:, pl.ds(j * WIDTH, WIDTH)] = c1o[j].astype(BF16)
            stage(j + 3)
            if j == 1:
                with scope('barrier'):
                    pl.semaphore_wait(bar, 4)
            if j >= 1:
                send_own(j - 1)
    send_own(nh - 1)
    for j in range(nf):
        for p in range(PIECES):
            src = gown.at[j, pl.ds(own + p * prow, prow)]
            dst = g_ref.at[j, pl.ds(oth + p * prow, prow)]
            remote(src, dst, yg_s, yg_r.at[j, p], yn).start()

    n_pieces = nf * PIECES

    def relay(k, offset, sem, recv, dev, forward):
        @pl.when((k >= 0) & (k < n_pieces))
        def _():
            j, p = lax.div(k, PIECES), lax.rem(k, PIECES)
            piece = g_ref.at[j, pl.ds(pl.multiple_of(offset + p * prow, prow), prow)]
            remote(piece, piece, sem, recv.at[j, p], dev).wait_recv()
            if forward:
                remote(piece, piece, xfwd_s, xfwd_r.at[j, p], xn).start()
            remote(piece, piece, cfar_s, core_r.at[nh + j], cn).start()

    def relay_y(*ks):
        for k in ks:
            with scope("relay_y"):
                relay(jnp.int32(k), own, yg_s, yg_r, yn, True)

    def relayed(j):
        return PIECES * j + 13 + lax.max(0, 6 - 4 * j)

    def relay_x(*ks):
        for k in ks:
            with scope("relay_x"):
                relay(jnp.int32(k), oth, xfwd_s, xfwd_r, xn, False)

    lent, borrowed = pl.ds((nh - 1) * WIDTH, WIDTH), pl.ds((2 * nh - 1) * WIDTH, WIDTH)

    def wait_core(q):
        with scope("wait_core"):
            both = gown.at[0, pl.ds(0, half)]
            remote(both, both, cfwd_s, core_r.at[q], cn).wait_recv()

    def col_copy(q):
        slot = lax.rem(q, 2)
        return pltpu.make_async_copy(g_ref.at[q - nh], gcol.at[slot], col_sem.at[slot])

    def k_rows(kg):
        return pl.ds(pl.multiple_of(kg * kg_rows, kg_rows), kg_rows)

    def tile_copy(kg, j):
        return pltpu.make_async_copy(g_ref.at[j, k_rows(kg)], gt.at[j], gt_sem.at[j])

    def loop(lo, hi, body):
        def go(i, carry):
            body(i)
            return carry
        lax.fori_loop(lo, hi, go, 0)

    def over_m(body):
        loop(0, rows // TILE_M, lambda i: body(pl.ds(pl.multiple_of(i * TILE_M, TILE_M), TILE_M)))

    def fold(v):
        return jnp.sum(v.reshape(-1, 8, WIDTH), axis=0)

    def unrolled(n, width, body):
        def some(i):
            for t in range(width):
                body(i * width + t)
        loop(0, n, some)

    def first_half(q):
        wait_core(q)

        c1[q] = dot(a0[:, :cols], gown[q, :half, :])

    def third_quarter(q):
        c1[q] += dot(a0[:, cols:cols + quad], gown[q, half:half + quad, :])

    def wait_a(i):
        with scope("wait_a"):
            part = a0.at[:, pl.ds(0, quad)]
            remote(part, part, ya_s, ya_r.at[i], yn).wait_recv()

    def early(j):
        with scope("wait_xown"):
            block = gown.at[j, theirs]
            remote(block, block, xown_s, xown_r.at[j], xn).wait_recv()
        remote(block, block, cfwd_s, core_r.at[j], cn).start()

        @pl.when(j >= 1)
        def _():
            with scope("first_half"):
                first_half(j - 1)

        @pl.when(j == nh - 3)
        def _():
            wait_a(0)

        @pl.when(j >= nh - 3)
        def _():
            with scope("third_quarter"):
                first = 2 * (j - (nh - 3))
                third_quarter(first)
                third_quarter(first + 1)
    loop(0, nh, early)
    relay_y(0)
    with scope("early_end"):
        third_quarter(nh - 2)
        first_half(nh - 1)
        third_quarter(nh - 1)
    relay_y(1, 2)
    wait_a(1)

    def add_other(kg, j, g_tile):
        c1o[j] += dot(a1[:, k_rows(kg)], g_tile[...])

    def finish(q, squares):
        with scope("finish"):
            three = sums.at[q, pl.ds(0, 3)]
            remote(three, three, sum_s, sum_r.at[q], cn).wait_recv()
            total = (sums[q, 0] + sums[q, 1]) + (sums[q, 2] + sums[q, 3])
            scale = n_all / total
            a1[:, chunk(q)] = (squares[...] * scale).astype(BF16)

    def send_sums(q):
        for dev in (cn, xn, dn):
            remote(sums.at[q, r], sums.at[q, r], sum_s, sum_r.at[q], dev).start()

    def own_expand(q):
        with scope("c0"):
            v = c1[q] + dot(a0[:, cols + quad:], gown[q, half + quad:, :])
            v = v * v
            c1[q] = v
            sums[q, r] = jnp.sum(fold(v), axis=0, keepdims=True)
        send_sums(q)
        for at, k in ((0, 3), (2, 4), (3, 5), (5, 6), (7, 7)):
            @pl.when(q == at)
            def _():
                relay_y(k)
    loop(0, nh, own_expand)

    def after(i, *relays):
        for at, k in relays:
            @pl.when(i == at)
            def _():
                relay_y(k)

    def own_finish(q):
        finish(q, c1.at[q])
        after(q, (1, 8), (3, 9), (7, 12))

    def own_first(n):
        with scope("own_first"):
            c1[n] = dot(a1[:, :quad], gown[n, :quad, :])
        after(n, (0, 10), (2, 11))

    def own_second(n):
        with scope("own_second"):
            c1[n] += dot(a1[:, quad:cols], gown[n, quad:half, :])
        after(n, (1, 13), (3, 14))

    def own_whole(n):
        with scope("own_whole"):
            c1[n] = dot(a1[:, :cols], gown[n, :half, :])
        relay_y(15 - nh // 2 + n)
    loop(0, nh // 2, own_finish)
    loop(0, nh // 2, own_first)
    loop(nh // 2, nh, own_finish)
    relay_x(0, 1, 2, 3, 4, 5, 6, 7)
    loop(0, nh // 2, own_second)
    remote(a1.at[:, lent], a1.at[:, borrowed], y1_s, y1_r, yn).start()
    wait_core(nh)
    col_copy(nh).start()
    loop(nh // 2, nh, own_whole)

    def right_own(kg):
        def some(i):
            for n in range(4):
                c1[4 * i + n] += dot(a1[:, k_rows(kg)], gown[4 * i + n, k_rows(kg), :])
        with scope("right_own"):
            loop(0, nh // 4, some)

    def right_one(q):
        k_one = chunk(q)

        def some(i):
            for n in range(4):
                c1[4 * i + n] += dot(a1[:, k_one], gown[4 * i + n, k_one, :])
        with scope("right_one"):
            loop(0, nh // 4, some)

    def right_other(kg, pairs):
        def pair(i):
            for j in (2 * i, 2 * i + 1):
                tile_copy(kg, j).wait()
            for j in (2 * i, 2 * i + 1):
                add_other(kg, j, gt.at[j])
        with scope("right_other"):
            loop(0, pairs, pair)

    def other_step(j):
        q = nh + j
        k = PIECES * j
        slot = lax.rem(q, 2)
        done = lax.div(q, 2)
        at_last = j == nf - 2
        paired = ((slot == 0) & (j > 0) & (j < nf - 1)) | at_last
        kg = lax.div(q - 1, 2)
        pairs = lax.div(j + 1, 2)
        ahead = relayed(j)

        def relay_ahead(*steps):
            for i in steps:
                @pl.when(ahead + i < relayed(j + 1))
                def _():
                    relay_y(ahead + i)

        def relay_next(*steps):
            for i in steps:
                relay_x(k + PIECES + i)
        with scope("load"):
            col_copy(q).wait()

        @pl.when(paired)
        def _():
            loop(0, 2 * pairs, lambda i: tile_copy(kg, i).start())
        relay_ahead(0)
        sums[q, r] = jnp.zeros((1, WIDTH), F32)

        def expand(m):
            v = dot(a0[m, :], gcol[slot])
            v = v * v
            mbuf[slot, m, :] = v
            sums[q, r] += jnp.sum(fold(v), axis=0, keepdims=True)
        with scope("c0"):
            over_m(expand)
        send_sums(q)
        relay_ahead(1, 2)
        relay_next(0, 1, 2)

        @pl.when((j > 0) & (j < nf - 1))
        def _():
            finish(q - 1, mbuf.at[1 - slot])

        def expand_flow(m):
            c1o[j, m, :] = dot(a1[m, :cols], gcol[slot, :half, :])
        with scope("left"):
            over_m(expand_flow)
            loop(nh // 2, done, lambda i: add_other(i, j, gcol.at[slot, k_rows(i)]))
        relay_ahead(3)
        relay_next(3, 4)

        @pl.when(at_last)
        def _():
            right_one(q - 1)
            finish(q, mbuf.at[slot])
            right_one(q)

        @pl.when(paired & ~at_last)
        def _():
            right_own(kg)
        relay_next(5)
        relay_ahead(4)
        relay_next(6)
        relay_ahead(5)
        relay_next(7)

        @pl.when(j + 1 < nf)
        def _():
            wait_core(q + 1)
            col_copy(q + 1).start()

        @pl.when(paired)
        def _():
            right_other(kg, pairs)
        relay_ahead(6, 7)
    loop(0, nf, other_step)

    last_kg = nh - 1
    loop(0, nf, lambda j: tile_copy(last_kg, j).start())
    finish(nc - 1, mbuf.at[(nc - 1) % 2])
    with scope("wait_a1"):
        remote(a1.at[:, lent], a1.at[:, borrowed], y1_s, y1_r, yn).wait()

    def close(c, i, part, g_tile):
        v = c[i] + dot(a1[:, k_rows(last_kg)], g_tile[...])
        v = v * v
        c[i] = v
        parts[part] = fold(v)

    def close_other(j):
        close(c1o, j, nh + j, gt.at[j])

    def send_s1(i):
        part = s1.at[i, r]
        for dev in (cn, xn, dn):
            remote(part, part, s1_s, s1_r.at[i], dev).start()

    with scope("close"):
        unrolled(nh // 4, 4, lambda n: close(c1, n, n, gown.at[n, k_rows(last_kg)]))
        s1[0, r] = jnp.sum(parts[:nh], axis=1)
    send_s1(0)
    with scope("close"):
        loop(0, nf, lambda j: tile_copy(last_kg, j).wait())
        unrolled(nh // 4, 4, close_other)
        s1[1, r] = jnp.sum(parts[nh:], axis=1)
    send_s1(1)

    def wait_s1(i):
        with scope("wait_s1"):
            three = s1.at[i, pl.ds(0, 3)]
            remote(three, three, s1_s, s1_r.at[i], cn).wait_recv()

    def rescale(i, n):
        line = pl.ds(n, 1)
        total = (s1[i, 0, line, :] + s1[i, 1, line, :]) + (s1[i, 2, line, :] + s1[i, 3, line, :])
        a0[:, chunk(i * nh + n)] = ((c1 if i == 0 else c1o)[n] * (n_all / total)).astype(BF16)

    remote(a0.at[:, pl.ds(0, cols)], a0.at[:, pl.ds(0, cols)], ya_s, ya_r.at[0], yn).wait_send()
    wait_s1(0)
    with scope("rescale"):
        loop(0, nh, lambda i: rescale(0, nh - 1 - i))

    near = nc * WIDTH

    def put(n, v):
        v = v * v
        c1[n] = v
        parts[n] = fold(v)

    def last_near(n):
        c1[n] = dot(a0[:, :cols], gown[n, :half, :])

    def last_other(n):
        c1[n] += dot(a0[:, cols:near], gown[n, half:near, :])

    def last(n):
        c1[n] = dot(a0[:, :near], gown[n, :near, :])

    def last_far(i):
        put(2 * i, c1[2 * i] + dot(a2[...], gown[2 * i, near:, :]))
        put(2 * i + 1, c1[2 * i + 1] + dot(a2[...], gown[2 * i + 1, near:, :]))

    def last_whole(n):
        put(n, dot(a0[:, :near], gown[n, :near, :]) + dot(a2[...], gown[n, near:, :]))
    with scope("last_near"):
        remote(a0.at[:, lent], a2, y2_s, y2_r, yn).start()
        loop(0, 2, last_near)
    wait_s1(1)
    with scope("rescale"):
        loop(0, nf, lambda n: rescale(1, n))
    with scope("last"):
        loop(0, 2, last_other)
        loop(2, nh - 2, last)
    with scope("wait_a2"):
        remote(a0.at[:, lent], a2, y2_s, y2_r, yn).wait()
    with scope("last_far"):
        loop(0, (nh - 2) // 2, last_far)
    with scope("last_whole"):
        loop(nh - 2, nh, last_whole)
        s2[r] = jnp.sum(parts[:nh], axis=1)

    for dev in (cn, xn, dn):
        remote(s2.at[r], s2.at[r], s2_s, s2_r, dev).start()

    def sent(ref, sem):
        remote(ref, ref, sem, s2_r, cn).wait_send()
    sent(gown.at[:, pl.ds(0, rows)], xown_s)
    sent(gown.at[pl.ds(0, nf), pl.ds(0, rows)], yg_s)
    sent(gown.at[:, pl.ds(0, rows)], cown_s)
    sent(gown.at[pl.ds(0, nf), pl.ds(0, rows)], xfwd_s)
    sent(gown.at[:, pl.ds(0, rows)], cfwd_s)
    sent(gown.at[pl.ds(0, nf), pl.ds(0, 2 * rows)], cfar_s)
    sent(sums.at[:, pl.ds(0, 3)], sum_s)
    sent(s1.at[:, pl.ds(0, 3)], s1_s)
    with scope("wait_s2"):
        three = s2.at[pl.ds(0, 3)]
        remote(three, three, s2_s, s2_r, cn).wait()
    total = (s2[0] + s2[1]) + (s2[2] + s2[3])
    for n in range(nh):
        sum_ref[:, n * WIDTH:(n + 1) * WIDTH] = total[n:n + 1]


def scale_kernel(n_all, raw_ref, sum_ref, out_ref, buf, out_sem):
    def put(i):
        return pltpu.make_async_copy(buf.at[i], out_ref.at[:, pl.ds(i * WIDTH, WIDTH)], out_sem.at[i])

    chunks = raw_ref.shape[0]
    for i in range(chunks):
        buf[i] = raw_ref[i] * (n_all / sum_ref[:, i * WIDTH:(i + 1) * WIDTH])
        put(i).start()
    for i in range(chunks):
        put(i).wait()


def solution(mesh):
    block_spec = P(("graph", "row"), "col")

    def device_step(init_blk, graph_blk):
        rows, cols = init_blk.shape
        n_all = 2 * cols
        nh = cols // WIDTH
        dma = pltpu.SemaphoreType.DMA
        any_spec, vmem_spec = pl.BlockSpec(memory_space=pl.ANY), pl.BlockSpec(memory_space=pltpu.VMEM)
        raw, col_sum, _ = pl.pallas_call(
            functools.partial(kernel, float(n_all)),
            out_shape=(
                pltpu.VMEM((nh, rows, WIDTH), F32),
                pltpu.VMEM((1, cols), F32),
                jax.ShapeDtypeStruct((nh - 1, n_all, WIDTH), BF16),
            ),
            in_specs=[any_spec, any_spec],
            out_specs=(vmem_spec, vmem_spec, any_spec),
            scratch_shapes=[
                pltpu.VMEM((rows, n_all), BF16),
                pltpu.VMEM((rows, n_all), BF16),
                pltpu.VMEM((rows, WIDTH), BF16),
                pltpu.VMEM((nh, rows, WIDTH), F32),
                pltpu.VMEM((2, rows, WIDTH), F32),
                pltpu.VMEM((nh, n_all, WIDTH), BF16),
                pltpu.VMEM((2, n_all, WIDTH), BF16),
                pltpu.VMEM((nh, 2 * WIDTH, WIDTH), BF16),
                pltpu.VMEM((2 * nh - 1, 4, 1, WIDTH), F32),
                pltpu.VMEM((2, 4, nh, WIDTH), F32),
                pltpu.VMEM((4, nh, WIDTH), F32),
                pltpu.VMEM((2 * nh, 8, WIDTH), F32),
                dma((2 * nh,)), dma((2,)), dma((nh,)),
                dma((nh,)), dma((nh, PIECES)), dma((2,)), dma((nh, PIECES)), dma, dma,
                dma((2 * nh,)), dma((2 * nh,)), dma((2,)), dma,
                dma, dma, dma, dma, dma, dma, dma, dma, dma, dma, dma, dma,
            ],
            compiler_params=pltpu.CompilerParams(
                collective_id=0, has_side_effects=True, vmem_limit_bytes=54 * 2**20),
            name="mcl",
        )(init_blk, graph_blk)
        return pl.pallas_call(
            functools.partial(scale_kernel, float(n_all)),
            out_shape=jax.ShapeDtypeStruct((rows, cols), F32),
            in_specs=[vmem_spec, vmem_spec],
            out_specs=any_spec,
            scratch_shapes=[pltpu.VMEM((nh, rows, WIDTH), F32), dma((nh,))],
            compiler_params=pltpu.CompilerParams(vmem_limit_bytes=40 * 2**20),
            name="scale",
        )(raw, col_sum)

    return jax.shard_map(device_step, mesh=mesh, in_specs=(block_spec, block_spec), out_specs=block_spec, check_vma=False)
```

```python
import contextlib
import functools

import jax
import jax.numpy as jnp
from jax import lax
from jax.experimental import pallas as pl
from jax.experimental.pallas import tpu as pltpu
from jax.sharding import PartitionSpec as P

MESH = pl.DeviceIdType.MESH
WIDTH = 256
PIECES = 8
TILE_M = 512
F32, BF16 = jnp.float32, jnp.bfloat16


def nothing(name):
    return contextlib.nullcontext()


scope = nothing


def dot(a, b):
    return jnp.dot(a, b, preferred_element_type=F32)


def kernel(n_all, flow_ref, graph_ref, c1, sum_ref, g_ref,
           a0, a1, a2, c1o, mbuf, gown, gcol, gt, sums, s1, s2, parts,
           stage_sem, col_sem, gt_sem,
           xown_r, xfwd_r, ya_r, yg_r, y1_r, y2_r, core_r, sum_r, s1_r, s2_r,
           xown_s, xfwd_s, ya_s, yg_s, y1_s, y2_s, cown_s, cfwd_s, cfar_s, sum_s, s1_s, s2_s):
    rows, cols = flow_ref.shape
    nh = cols // WIDTH
    nf = nh - 1
    nc = nh + nf
    depth = 4 * rows
    half = depth // 2
    quad = half // 2
    kg_rows = 2 * WIDTH
    prow = rows // PIECES

    y = lax.axis_index("col")
    r = lax.axis_index("row")
    z = lax.axis_index("graph")
    x = lax.div(r, 2)
    c = lax.rem(r, 2)
    xn = (z, y, (1 - x) * 2 + c)
    yn = (z, 1 - y, r)
    cn = (z, y, x * 2 + 1 - c)
    dn = (z, y, (1 - x) * 2 + 1 - c)
    lx = x + y - 2 * x * y
    own = pl.multiple_of((lx * 2 + c) * rows, rows)
    oth = pl.multiple_of(((1 - lx) * 2 + c) * rows, rows)
    mine, theirs = pl.ds(own, rows), pl.ds(oth, rows)

    def remote(src, dst, send, recv, dev):
        return pltpu.make_async_remote_copy(
            src_ref=src, dst_ref=dst, send_sem=send, recv_sem=recv, device_id=dev, device_id_type=MESH)

    def chunk(q):
        return pl.ds(pl.multiple_of(q * WIDTH, WIDTH), WIDTH)

    def stage_copy(k):
        src = graph_ref if k < nh else flow_ref
        return pltpu.make_async_copy(src.at[:, pl.ds((k % nh) * WIDTH, WIDTH)],
                                     c1.at[k] if k < nh else c1o.at[k - nh], stage_sem.at[k])

    def stage(j):
        if j < nh:
            stage_copy(nh + j).start()
            stage_copy(j).start()

    gt[nh - 1] = jnp.zeros((kg_rows, WIDTH), BF16)
    stage(0)
    bar = pltpu.get_barrier_semaphore()
    for dev in (xn, yn, cn, dn):
        pl.semaphore_signal(bar, inc=1, device_id=dev, device_id_type=MESH)
    stage(1)
    stage(2)

    def send_graph(j):
        block = gown.at[j, mine]
        remote(block, block, xown_s, xown_r.at[j], xn).start()
        remote(block, block, cown_s, core_r.at[j], cn).start()

    def send_flow(j):
        piece = pl.ds(j * WIDTH, WIDTH)
        remote(a0.at[:, piece], a0.at[:, pl.ds(cols + j * WIDTH, WIDTH)], ya_s, ya_r.at[j * 2 // nh], yn).start()

    with scope("cast"):
        for j in range(nh):
            stage_copy(nh + j).wait()
            a0[:, pl.ds(j * WIDTH, WIDTH)] = c1o[j].astype(BF16)
            if j >= 1:
                send_graph(j - 1)
            stage_copy(j).wait()
            gown[j, mine, :] = c1[j].astype(BF16)
            if j == 0:
                with scope("barrier"):
                    pl.semaphore_wait(bar, 4)
            send_flow(j)
            stage(j + 3)
    send_graph(nh - 1)
    for j in range(nf):
        for p in range(PIECES):
            src = gown.at[j, pl.ds(own + p * prow, prow)]
            dst = g_ref.at[j, pl.ds(oth + p * prow, prow)]
            remote(src, dst, yg_s, yg_r.at[j, p], yn).start()

    n_pieces = nf * PIECES

    def relay(k, offset, sem, recv, dev, forward):
        @pl.when((k >= 0) & (k < n_pieces))
        def _():
            j, p = lax.div(k, PIECES), lax.rem(k, PIECES)
            piece = g_ref.at[j, pl.ds(pl.multiple_of(offset + p * prow, prow), prow)]
            remote(piece, piece, sem, recv.at[j, p], dev).wait_recv()
            if forward:
                remote(piece, piece, xfwd_s, xfwd_r.at[j, p], xn).start()
            remote(piece, piece, cfar_s, core_r.at[nh + j], cn).start()

    def relay_y(*ks):
        for k in ks:
            with scope("relay_y"):
                relay(jnp.int32(k), own, yg_s, yg_r, yn, True)

    def relayed(j):
        return PIECES * j + 13 + lax.max(lax.max(0, 5 - 3 * j), 2 - 2 * lax.abs(j - 2))

    def relay_x(*ks):
        for k in ks:
            with scope("relay_x"):
                relay(jnp.int32(k), oth, xfwd_s, xfwd_r, xn, False)

    lent, borrowed = pl.ds((nh - 1) * WIDTH, WIDTH), pl.ds((2 * nh - 1) * WIDTH, WIDTH)

    def wait_core(q):
        with scope("wait_core"):
            both = gown.at[0, pl.ds(0, half)]
            remote(both, both, cfwd_s, core_r.at[q], cn).wait_recv()

    def col_copy(q):
        slot = lax.rem(q, 2)
        return pltpu.make_async_copy(g_ref.at[q - nh], gcol.at[slot], col_sem.at[slot])

    def k_rows(kg):
        return pl.ds(pl.multiple_of(kg * kg_rows, kg_rows), kg_rows)

    def tile_copy(kg, j):
        return pltpu.make_async_copy(g_ref.at[j, k_rows(kg)], gt.at[j], gt_sem.at[j])

    def loop(lo, hi, body):
        def go(i, carry):
            body(i)
            return carry
        lax.fori_loop(lo, hi, go, 0)

    def over_m(body):
        loop(0, rows // TILE_M, lambda i: body(pl.ds(pl.multiple_of(i * TILE_M, TILE_M), TILE_M)))

    def fold(v):
        return jnp.sum(v.reshape(-1, 8, WIDTH), axis=0)

    def unrolled(n, width, body):
        def some(i):
            for t in range(width):
                body(i * width + t)
        loop(0, n, some)

    def first_half(q):
        wait_core(q)

        c1[q] = dot(a0[:, :cols], gown[q, :half, :])

    def third_quarter(q):
        c1[q] += dot(a0[:, cols:cols + quad], gown[q, half:half + quad, :])

    def wait_a(i):
        with scope("wait_a"):
            part = a0.at[:, pl.ds(0, quad)]
            remote(part, part, ya_s, ya_r.at[i], yn).wait_recv()

    def early(j):
        with scope("wait_xown"):
            block = gown.at[j, theirs]
            remote(block, block, xown_s, xown_r.at[j], xn).wait_recv()
        remote(block, block, cfwd_s, core_r.at[j], cn).start()

        @pl.when(j >= 1)
        def _():
            with scope("first_half"):
                first_half(j - 1)

        @pl.when(j == nh - 3)
        def _():
            wait_a(0)

            with scope("third_quarter"):
                loop(0, nh - 3, third_quarter)

        @pl.when(j > nh - 3)
        def _():
            with scope("third_quarter"):
                third_quarter(j - 1)
    loop(0, nh, early)
    relay_y(0)
    with scope("early_end"):
        first_half(nh - 1)
    relay_y(1)
    with scope("early_end"):
        third_quarter(nh - 1)
    wait_a(1)

    def add_other(kg, j, g_tile):
        c1o[j] += dot(a1[:, k_rows(kg)], g_tile[...])

    def finish(q, squares):
        with scope("finish"):
            three = sums.at[q, pl.ds(0, 3)]
            remote(three, three, sum_s, sum_r.at[q], cn).wait_recv()
            total = (sums[q, 0] + sums[q, 1]) + (sums[q, 2] + sums[q, 3])
            scale = n_all / total
            a1[:, chunk(q)] = (squares[...] * scale).astype(BF16)

    def send_sums(q):
        for dev in (cn, xn, dn):
            remote(sums.at[q, r], sums.at[q, r], sum_s, sum_r.at[q], dev).start()

    def own_expand(q):
        with scope("c0"):
            v = c1[q] + dot(a0[:, cols + quad:], gown[q, half + quad:, :])
            v = v * v
            c1[q] = v
            sums[q, r] = jnp.sum(fold(v), axis=0, keepdims=True)
        send_sums(q)
        for at, k in ((0, 2), (2, 3), (3, 4), (5, 5), (7, 6)):
            @pl.when(q == at)
            def _():
                relay_y(k)
    loop(0, nh, own_expand)

    def after(i, *relays):
        for at, k in relays:
            @pl.when(i == at)
            def _():
                relay_y(k)

    def own_finish(q):
        finish(q, c1.at[q])
        after(q, (1, 7), (3, 8), (5, 11))

    def own_first(n):
        with scope("own_first"):
            c1[n] = dot(a1[:, :quad], gown[n, :quad, :])
        after(n, (0, 9), (2, 10))

    def own_second(n):
        with scope("own_second"):
            c1[n] += dot(a1[:, quad:cols], gown[n, quad:half, :])
        after(n, (0, 12), (2, 13))

    def own_whole(n):
        with scope("own_whole"):
            c1[n] = dot(a1[:, :cols], gown[n, :half, :])
        relay_y(14 - nh // 2 + n)
    loop(0, nh // 2, own_finish)
    loop(0, nh // 2, own_first)
    loop(nh // 2, nh, own_finish)
    relay_x(0, 1, 2, 3, 4, 5, 6, 7)
    loop(0, nh // 2, own_second)
    remote(a1.at[:, lent], a1.at[:, borrowed], y1_s, y1_r, yn).start()
    wait_core(nh)
    col_copy(nh).start()
    loop(nh // 2, nh, own_whole)

    def right_one(q):
        k_one = chunk(q)

        def some(i):
            for n in range(4):
                c1[4 * i + n] += dot(a1[:, k_one], gown[4 * i + n, k_one, :])
        with scope("right_one"):
            loop(0, nh // 4, some)

    def right_other(kg, pairs):
        def pair(i):
            for j in (2 * i, 2 * i + 1):
                tile_copy(kg, j).wait()
            for j in (2 * i, 2 * i + 1):
                add_other(kg, j, gt.at[j])
        with scope("right_other"):
            loop(0, pairs, pair)

    def other_step(j):
        q = nh + j
        k = PIECES * j
        slot = lax.rem(q, 2)
        done = lax.div(q, 2)
        paired = slot == 1
        kg = lax.div(q - 1, 2)
        pairs = lax.div(j + 1, 2)
        ahead = relayed(j)

        def relay_ahead(*steps):
            for i in steps:
                @pl.when(ahead + i < relayed(j + 1))
                def _():
                    relay_y(ahead + i)

        def relay_next(*steps):
            for i in steps:
                relay_x(k + PIECES + i)
        with scope("load"):
            col_copy(q).wait()

        @pl.when(paired)
        def _():
            loop(0, 2 * pairs, lambda i: tile_copy(kg, i).start())
        relay_ahead(0)
        sums[q, r] = jnp.zeros((1, WIDTH), F32)

        def expand(m):
            v = dot(a0[m, :], gcol[slot])
            v = v * v
            mbuf[slot, m, :] = v
            sums[q, r] += jnp.sum(fold(v), axis=0, keepdims=True)
        with scope("c0"):
            over_m(expand)
        send_sums(q)
        relay_ahead(1, 2)
        relay_next(0, 1, 2)

        @pl.when(paired)
        def _():
            finish(q - 1, mbuf.at[1 - slot])

        def expand_flow(m):
            c1o[j, m, :] = dot(a1[m, :cols], gcol[slot, :half, :])
        with scope("left"):
            over_m(expand_flow)
            loop(nh // 2, done, lambda i: add_other(i, j, gcol.at[slot, k_rows(i)]))
        relay_ahead(3)
        relay_next(3, 4)

        @pl.when(paired)
        def _():
            right_one(q - 1)
            relay_ahead(4)
            finish(q, mbuf.at[slot])
            right_one(q)
            relay_ahead(5)
            relay_next(5, 6, 7)

        @pl.when(~paired)
        def _():
            relay_next(5)
            relay_ahead(4)
            relay_next(6)
            relay_ahead(5)
            relay_next(7)

        relay_ahead(6)

        @pl.when(j + 1 < nf)
        def _():
            wait_core(q + 1)
            col_copy(q + 1).start()
        relay_ahead(7)

        @pl.when(paired)
        def _():
            right_other(kg, pairs)
    loop(0, nf, other_step)

    last_kg = nh - 1
    loop(0, nf, lambda j: tile_copy(last_kg, j).start())
    finish(nc - 1, mbuf.at[(nc - 1) % 2])
    with scope("wait_a1"):
        remote(a1.at[:, lent], a1.at[:, borrowed], y1_s, y1_r, yn).wait()

    def close(c, i, part, g_tile):
        v = c[i] + dot(a1[:, k_rows(last_kg)], g_tile[...])
        v = v * v
        c[i] = v
        parts[part] = fold(v)

    def close_other(j):
        close(c1o, j, nh + j, gt.at[j])

    def send_s1(i):
        part = s1.at[i, r]
        for dev in (cn, xn, dn):
            remote(part, part, s1_s, s1_r.at[i], dev).start()

    with scope("close"):
        unrolled(nh // 4, 4, lambda n: close(c1, n, n, gown.at[n, k_rows(last_kg)]))
        s1[0, r] = jnp.sum(parts[:nh], axis=1)
    send_s1(0)
    with scope("close"):
        loop(0, nf, lambda j: tile_copy(last_kg, j).wait())
        unrolled(nh // 4, 4, close_other)
        s1[1, r] = jnp.sum(parts[nh:], axis=1)
    send_s1(1)

    def wait_s1(i):
        with scope("wait_s1"):
            three = s1.at[i, pl.ds(0, 3)]
            remote(three, three, s1_s, s1_r.at[i], cn).wait_recv()

    def rescale(i, n):
        line = pl.ds(n, 1)
        total = (s1[i, 0, line, :] + s1[i, 1, line, :]) + (s1[i, 2, line, :] + s1[i, 3, line, :])
        a0[:, chunk(i * nh + n)] = ((c1 if i == 0 else c1o)[n] * (n_all / total)).astype(BF16)

    remote(a0.at[:, pl.ds(0, cols)], a0.at[:, pl.ds(0, cols)], ya_s, ya_r.at[0], yn).wait_send()
    wait_s1(0)
    with scope("rescale"):
        loop(0, nh, lambda i: rescale(0, nh - 1 - i))

    near = nc * WIDTH

    def put(n, v):
        v = v * v
        c1[n] = v
        parts[n] = fold(v)

    def last_near(n):
        c1[n] = dot(a0[:, :cols], gown[n, :half, :])

    def last_other(n):
        c1[n] += dot(a0[:, cols:near], gown[n, half:near, :])

    def last(n):
        c1[n] = dot(a0[:, :near], gown[n, :near, :])

    def last_far(i):
        put(2 * i, c1[2 * i] + dot(a2[...], gown[2 * i, near:, :]))
        put(2 * i + 1, c1[2 * i + 1] + dot(a2[...], gown[2 * i + 1, near:, :]))

    def last_whole(n):
        put(n, dot(a0[:, :near], gown[n, :near, :]) + dot(a2[...], gown[n, near:, :]))
    with scope("last_near"):
        remote(a0.at[:, lent], a2, y2_s, y2_r, yn).start()
        loop(0, 2, last_near)
    wait_s1(1)
    with scope("rescale"):
        loop(0, nf, lambda n: rescale(1, n))
    with scope("last"):
        loop(0, 2, last_other)
        loop(2, nh - 2, last)
    with scope("wait_a2"):
        remote(a0.at[:, lent], a2, y2_s, y2_r, yn).wait()
    with scope("last_far"):
        loop(0, (nh - 2) // 2, last_far)
    with scope("last_whole"):
        loop(nh - 2, nh, last_whole)
        s2[r] = jnp.sum(parts[:nh], axis=1)

    for dev in (cn, xn, dn):
        remote(s2.at[r], s2.at[r], s2_s, s2_r, dev).start()

    def sent(ref, sem):
        remote(ref, ref, sem, s2_r, cn).wait_send()
    sent(gown.at[:, pl.ds(0, rows)], xown_s)
    sent(gown.at[pl.ds(0, nf), pl.ds(0, rows)], yg_s)
    sent(gown.at[:, pl.ds(0, rows)], cown_s)
    sent(gown.at[pl.ds(0, nf), pl.ds(0, rows)], xfwd_s)
    sent(gown.at[:, pl.ds(0, rows)], cfwd_s)
    sent(gown.at[pl.ds(0, nf), pl.ds(0, 2 * rows)], cfar_s)
    sent(sums.at[:, pl.ds(0, 3)], sum_s)
    sent(s1.at[:, pl.ds(0, 3)], s1_s)
    with scope("wait_s2"):
        three = s2.at[pl.ds(0, 3)]
        remote(three, three, s2_s, s2_r, cn).wait()
    total = (s2[0] + s2[1]) + (s2[2] + s2[3])
    for n in range(nh):
        sum_ref[:, n * WIDTH:(n + 1) * WIDTH] = total[n:n + 1]


def scale_kernel(n_all, raw_ref, sum_ref, out_ref, buf, out_sem):
    def put(i):
        return pltpu.make_async_copy(buf.at[i], out_ref.at[:, pl.ds(i * WIDTH, WIDTH)], out_sem.at[i])

    chunks = raw_ref.shape[0]
    for i in range(chunks):
        buf[i] = raw_ref[i] * (n_all / sum_ref[:, i * WIDTH:(i + 1) * WIDTH])
        put(i).start()
    for i in range(chunks):
        put(i).wait()


def solution(mesh):
    block_spec = P(("graph", "row"), "col")

    def device_step(init_blk, graph_blk):
        rows, cols = init_blk.shape
        n_all = 2 * cols
        nh = cols // WIDTH
        dma = pltpu.SemaphoreType.DMA
        any_spec, vmem_spec = pl.BlockSpec(memory_space=pl.ANY), pl.BlockSpec(memory_space=pltpu.VMEM)
        raw, col_sum, _ = pl.pallas_call(
            functools.partial(kernel, float(n_all)),
            out_shape=(
                pltpu.VMEM((nh, rows, WIDTH), F32),
                pltpu.VMEM((1, cols), F32),
                jax.ShapeDtypeStruct((nh - 1, n_all, WIDTH), BF16),
            ),
            in_specs=[any_spec, any_spec],
            out_specs=(vmem_spec, vmem_spec, any_spec),
            scratch_shapes=[
                pltpu.VMEM((rows, n_all), BF16),
                pltpu.VMEM((rows, n_all), BF16),
                pltpu.VMEM((rows, WIDTH), BF16),
                pltpu.VMEM((nh, rows, WIDTH), F32),
                pltpu.VMEM((2, rows, WIDTH), F32),
                pltpu.VMEM((nh, n_all, WIDTH), BF16),
                pltpu.VMEM((2, n_all, WIDTH), BF16),
                pltpu.VMEM((nh, 2 * WIDTH, WIDTH), BF16),
                pltpu.VMEM((2 * nh - 1, 4, 1, WIDTH), F32),
                pltpu.VMEM((2, 4, nh, WIDTH), F32),
                pltpu.VMEM((4, nh, WIDTH), F32),
                pltpu.VMEM((2 * nh, 8, WIDTH), F32),
                dma((2 * nh,)), dma((2,)), dma((nh,)),
                dma((nh,)), dma((nh, PIECES)), dma((2,)), dma((nh, PIECES)), dma, dma,
                dma((2 * nh,)), dma((2 * nh,)), dma((2,)), dma,
                dma, dma, dma, dma, dma, dma, dma, dma, dma, dma, dma, dma,
            ],
            compiler_params=pltpu.CompilerParams(
                collective_id=0, has_side_effects=True, vmem_limit_bytes=54 * 2**20),
            name="mcl",
        )(init_blk, graph_blk)
        return pl.pallas_call(
            functools.partial(scale_kernel, float(n_all)),
            out_shape=jax.ShapeDtypeStruct((rows, cols), F32),
            in_specs=[vmem_spec, vmem_spec],
            out_specs=any_spec,
            scratch_shapes=[pltpu.VMEM((nh, rows, WIDTH), F32), dma((nh,))],
            compiler_params=pltpu.CompilerParams(vmem_limit_bytes=40 * 2**20),
            name="scale",
        )(raw, col_sum)

    return jax.shard_map(device_step, mesh=mesh, in_specs=(block_spec, block_spec), out_specs=block_spec, check_vma=False)
```

```python
import contextlib
import functools

import jax
import jax.numpy as jnp
from jax import lax
from jax.experimental import pallas as pl
from jax.experimental.pallas import tpu as pltpu
from jax.sharding import PartitionSpec as P

MESH = pl.DeviceIdType.MESH
WIDTH = 256
PIECES = 8
TILE_M = 512
F32, BF16 = jnp.float32, jnp.bfloat16


def nothing(name):
    return contextlib.nullcontext()


scope = nothing


def dot(a, b):
    return jnp.dot(a, b, preferred_element_type=F32)


def kernel(n_all, flow_ref, graph_ref, c1, sum_ref, g_ref,
           a0, a1, a2, c1o, mbuf, gown, gcol, gt, sums, s1, s2, parts,
           stage_sem, col_sem, gt_sem,
           xown_r, xfwd_r, ya_r, yg_r, y1_r, y2_r, core_r, sum_r, s1_r, s2_r,
           xown_s, xfwd_s, ya_s, yg_s, y1_s, y2_s, cown_s, cfwd_s, cfar_s, sum_s, s1_s, s2_s):
    rows, cols = flow_ref.shape
    nh = cols // WIDTH
    nf = nh - 1
    nc = nh + nf
    depth = 4 * rows
    half = depth // 2
    quad = half // 2
    kg_rows = 2 * WIDTH
    prow = rows // PIECES

    y = lax.axis_index("col")
    r = lax.axis_index("row")
    z = lax.axis_index("graph")
    x = lax.div(r, 2)
    c = lax.rem(r, 2)
    xn = (z, y, (1 - x) * 2 + c)
    yn = (z, 1 - y, r)
    cn = (z, y, x * 2 + 1 - c)
    dn = (z, y, (1 - x) * 2 + 1 - c)
    lx = x + y - 2 * x * y
    own = pl.multiple_of((lx * 2 + c) * rows, rows)
    oth = pl.multiple_of(((1 - lx) * 2 + c) * rows, rows)
    mine, theirs = pl.ds(own, rows), pl.ds(oth, rows)

    def remote(src, dst, send, recv, dev):
        return pltpu.make_async_remote_copy(
            src_ref=src, dst_ref=dst, send_sem=send, recv_sem=recv, device_id=dev, device_id_type=MESH)

    def chunk(q):
        return pl.ds(pl.multiple_of(q * WIDTH, WIDTH), WIDTH)

    def stage_copy(k):
        src = graph_ref if k < nh else flow_ref
        return pltpu.make_async_copy(src.at[:, pl.ds((k % nh) * WIDTH, WIDTH)],
                                     c1.at[k] if k < nh else c1o.at[k - nh], stage_sem.at[k])

    def stage(j):
        if j < nh:
            stage_copy(nh + j).start()
            stage_copy(j).start()

    gt[nh - 1] = jnp.zeros((kg_rows, WIDTH), BF16)
    stage(0)
    bar = pltpu.get_barrier_semaphore()
    for dev in (xn, yn, cn, dn):
        pl.semaphore_signal(bar, inc=1, device_id=dev, device_id_type=MESH)
    stage(1)
    stage(2)

    def send_graph(j):
        block = gown.at[j, mine]
        remote(block, block, xown_s, xown_r.at[j], xn).start()
        remote(block, block, cown_s, core_r.at[j], cn).start()

    def send_flow(j):
        piece = pl.ds(j * WIDTH, WIDTH)
        remote(a0.at[:, piece], a0.at[:, pl.ds(cols + j * WIDTH, WIDTH)], ya_s, ya_r.at[j * 2 // nh], yn).start()

    with scope("cast"):
        for j in range(nh):
            stage_copy(nh + j).wait()
            a0[:, pl.ds(j * WIDTH, WIDTH)] = c1o[j].astype(BF16)
            if j >= 1:
                send_graph(j - 1)
            stage_copy(j).wait()
            gown[j, mine, :] = c1[j].astype(BF16)
            if j == 0:
                with scope("barrier"):
                    pl.semaphore_wait(bar, 4)
            send_flow(j)
            stage(j + 3)
    send_graph(nh - 1)
    for j in range(nf):
        for p in range(PIECES):
            src = gown.at[j, pl.ds(own + p * prow, prow)]
            dst = g_ref.at[j, pl.ds(oth + p * prow, prow)]
            remote(src, dst, yg_s, yg_r.at[j, p], yn).start()

    n_pieces = nf * PIECES

    def relay(k, offset, sem, recv, dev, forward):
        @pl.when((k >= 0) & (k < n_pieces))
        def _():
            j, p = lax.div(k, PIECES), lax.rem(k, PIECES)
            piece = g_ref.at[j, pl.ds(pl.multiple_of(offset + p * prow, prow), prow)]
            remote(piece, piece, sem, recv.at[j, p], dev).wait_recv()
            if forward:
                remote(piece, piece, xfwd_s, xfwd_r.at[j, p], xn).start()
            remote(piece, piece, cfar_s, core_r.at[nh + j], cn).start()

    def relay_y(*ks):
        for k in ks:
            with scope("relay_y"):
                relay(jnp.int32(k), own, yg_s, yg_r, yn, True)

    def relayed(j):
        return PIECES * j + 13 + lax.max(lax.max(0, 5 - 3 * j), 2 - 2 * lax.abs(j - 2))

    def relay_x(*ks):
        for k in ks:
            with scope("relay_x"):
                relay(jnp.int32(k), oth, xfwd_s, xfwd_r, xn, False)

    lent, borrowed = pl.ds((nh - 1) * WIDTH, WIDTH), pl.ds((2 * nh - 1) * WIDTH, WIDTH)

    def wait_core(q):
        with scope("wait_core"):
            both = gown.at[0, pl.ds(0, half)]
            remote(both, both, cfwd_s, core_r.at[q], cn).wait_recv()

    def col_copy(q):
        slot = lax.rem(q, 2)
        return pltpu.make_async_copy(g_ref.at[q - nh], gcol.at[slot], col_sem.at[slot])

    def k_rows(kg):
        return pl.ds(pl.multiple_of(kg * kg_rows, kg_rows), kg_rows)

    def tile_copy(kg, j):
        return pltpu.make_async_copy(g_ref.at[j, k_rows(kg)], gt.at[j], gt_sem.at[j])

    def loop(lo, hi, body):
        def go(i, carry):
            body(i)
            return carry
        lax.fori_loop(lo, hi, go, 0)

    def over_m(body):
        loop(0, rows // TILE_M, lambda i: body(pl.ds(pl.multiple_of(i * TILE_M, TILE_M), TILE_M)))

    def fold(v):
        return jnp.sum(v.reshape(-1, 8, WIDTH), axis=0)

    def unrolled(n, width, body):
        def some(i):
            for t in range(width):
                body(i * width + t)
        loop(0, n, some)

    def first_half(q):
        wait_core(q)

        c1[q] = dot(a0[:, :cols], gown[q, :half, :])

    def third_quarter(q):
        c1[q] += dot(a0[:, cols:cols + quad], gown[q, half:half + quad, :])

    def wait_a(i):
        with scope("wait_a"):
            part = a0.at[:, pl.ds(0, quad)]
            remote(part, part, ya_s, ya_r.at[i], yn).wait_recv()

    def early(j):
        with scope("wait_xown"):
            block = gown.at[j, theirs]
            remote(block, block, xown_s, xown_r.at[j], xn).wait_recv()
        remote(block, block, cfwd_s, core_r.at[j], cn).start()

        @pl.when(j >= 1)
        def _():
            with scope("first_half"):
                first_half(j - 1)

        @pl.when(j == nh - 3)
        def _():
            wait_a(0)

            with scope("third_quarter"):
                loop(0, nh - 3, third_quarter)

        @pl.when(j > nh - 3)
        def _():
            with scope("third_quarter"):
                third_quarter(j - 1)
    loop(0, nh, early)
    relay_y(0)
    with scope("early_end"):
        first_half(nh - 1)
    relay_y(1)
    with scope("early_end"):
        third_quarter(nh - 1)
    wait_a(1)

    def add_other(kg, j, g_tile):
        c1o[j] += dot(a1[:, k_rows(kg)], g_tile[...])

    def finish(q, squares):
        with scope("finish"):
            three = sums.at[q, pl.ds(0, 3)]
            remote(three, three, sum_s, sum_r.at[q], cn).wait_recv()
            total = (sums[q, 0] + sums[q, 1]) + (sums[q, 2] + sums[q, 3])
            scale = n_all / total
            a1[:, chunk(q)] = (squares[...] * scale).astype(BF16)

    def send_sums(q):
        for dev in (cn, xn, dn):
            remote(sums.at[q, r], sums.at[q, r], sum_s, sum_r.at[q], dev).start()

    def own_expand(q):
        with scope("c0"):
            v = c1[q] + dot(a0[:, cols + quad:], gown[q, half + quad:, :])
            v = v * v
            c1[q] = v
            sums[q, r] = jnp.sum(fold(v), axis=0, keepdims=True)
        send_sums(q)
        for at, k in ((0, 2), (2, 3), (3, 4), (5, 5), (7, 6)):
            @pl.when(q == at)
            def _():
                relay_y(k)
    loop(0, nh, own_expand)

    def after(i, *relays):
        for at, k in relays:
            @pl.when(i == at)
            def _():
                relay_y(k)

    def own_finish(q):
        finish(q, c1.at[q])
        after(q, (1, 7), (3, 8), (5, 11))

    def own_first(n):
        with scope("own_first"):
            c1[n] = dot(a1[:, :quad], gown[n, :quad, :])
        after(n, (0, 9), (2, 10))

    def own_second(n):
        with scope("own_second"):
            c1[n] += dot(a1[:, quad:cols], gown[n, quad:half, :])
        after(n, (0, 12), (2, 13))

    def own_whole(n):
        with scope("own_whole"):
            c1[n] = dot(a1[:, :cols], gown[n, :half, :])
        relay_y(14 - nh // 2 + n)
    loop(0, nh // 2, own_finish)
    loop(0, nh // 2, own_first)
    loop(nh // 2, nh, own_finish)
    relay_x(0, 1, 2, 3, 4, 5, 6, 7)
    loop(0, nh // 2, own_second)
    remote(a1.at[:, lent], a1.at[:, borrowed], y1_s, y1_r, yn).start()
    wait_core(nh)
    col_copy(nh).start()
    loop(nh // 2, nh, own_whole)

    def right_one(q):
        k_one = chunk(q)

        def some(i):
            for n in range(4):
                c1[4 * i + n] += dot(a1[:, k_one], gown[4 * i + n, k_one, :])
        with scope("right_one"):
            loop(0, nh // 4, some)

    def right_other(kg, pairs):
        def pair(i):
            for j in (2 * i, 2 * i + 1):
                tile_copy(kg, j).wait()
            for j in (2 * i, 2 * i + 1):
                add_other(kg, j, gt.at[j])
        with scope("right_other"):
            loop(0, pairs, pair)

    def other_step(j):
        q = nh + j
        k = PIECES * j
        slot = lax.rem(q, 2)
        done = lax.div(q, 2)
        paired = slot == 1
        kg = lax.div(q - 1, 2)
        pairs = lax.div(j + 1, 2)
        ahead = relayed(j)

        def relay_ahead(*steps):
            for i in steps:
                @pl.when(ahead + i < relayed(j + 1))
                def _():
                    relay_y(ahead + i)

        def relay_next(*steps):
            for i in steps:
                relay_x(k + PIECES + i)
        with scope("load"):
            col_copy(q).wait()

        @pl.when(paired)
        def _():
            loop(0, 2 * pairs, lambda i: tile_copy(kg, i).start())
        relay_ahead(0)
        sums[q, r] = jnp.zeros((1, WIDTH), F32)

        def expand(m):
            v = dot(a0[m, :], gcol[slot])
            v = v * v
            mbuf[slot, m, :] = v
            sums[q, r] += jnp.sum(fold(v), axis=0, keepdims=True)
        with scope("c0"):
            over_m(expand)
        send_sums(q)
        relay_ahead(1, 2)
        relay_next(0, 1, 2)

        @pl.when(paired)
        def _():
            finish(q - 1, mbuf.at[1 - slot])

        def expand_flow(m):
            c1o[j, m, :] = dot(a1[m, :cols], gcol[slot, :half, :])
        with scope("left"):
            over_m(expand_flow)
            twos = lax.div(done - nh // 2, 2)

            def two(i):
                k = pl.ds(pl.multiple_of(cols + i * 2 * kg_rows, 2 * kg_rows), 2 * kg_rows)
                c1o[j] += dot(a1[:, k], gcol[slot, k, :])
            loop(0, twos, two)
            loop(nh // 2 + 2 * twos, done, lambda i: add_other(i, j, gcol.at[slot, k_rows(i)]))
        relay_ahead(3)
        relay_next(3, 4)

        @pl.when(paired)
        def _():
            right_one(q - 1)
            relay_ahead(4)
            finish(q, mbuf.at[slot])
            right_one(q)
            relay_ahead(5)
            relay_next(5, 6, 7)

        @pl.when(~paired)
        def _():
            relay_next(5)
            relay_ahead(4)
            relay_next(6)
            relay_ahead(5)
            relay_next(7)

        relay_ahead(6)

        @pl.when(j + 1 < nf)
        def _():
            wait_core(q + 1)
            col_copy(q + 1).start()
        relay_ahead(7)

        @pl.when(paired)
        def _():
            right_other(kg, pairs)
    loop(0, nf, other_step)

    last_kg = nh - 1
    loop(0, nf, lambda j: tile_copy(last_kg, j).start())
    finish(nc - 1, mbuf.at[(nc - 1) % 2])
    with scope("wait_a1"):
        remote(a1.at[:, lent], a1.at[:, borrowed], y1_s, y1_r, yn).wait()

    def close(c, i, part, g_tile):
        v = c[i] + dot(a1[:, k_rows(last_kg)], g_tile[...])
        v = v * v
        c[i] = v
        parts[part] = fold(v)

    def close_other(j):
        close(c1o, j, nh + j, gt.at[j])

    def send_s1(i):
        part = s1.at[i, r]
        for dev in (cn, xn, dn):
            remote(part, part, s1_s, s1_r.at[i], dev).start()

    with scope("close"):
        unrolled(nh // 4, 4, lambda n: close(c1, n, n, gown.at[n, k_rows(last_kg)]))
        s1[0, r] = jnp.sum(parts[:nh], axis=1)
    send_s1(0)
    with scope("close"):
        loop(0, nf, lambda j: tile_copy(last_kg, j).wait())
        unrolled(nh // 4, 4, close_other)
        s1[1, r] = jnp.sum(parts[nh:], axis=1)
    send_s1(1)

    def wait_s1(i):
        with scope("wait_s1"):
            three = s1.at[i, pl.ds(0, 3)]
            remote(three, three, s1_s, s1_r.at[i], cn).wait_recv()

    def rescale(i, n):
        line = pl.ds(n, 1)
        total = (s1[i, 0, line, :] + s1[i, 1, line, :]) + (s1[i, 2, line, :] + s1[i, 3, line, :])
        a0[:, chunk(i * nh + n)] = ((c1 if i == 0 else c1o)[n] * (n_all / total)).astype(BF16)

    remote(a0.at[:, pl.ds(0, cols)], a0.at[:, pl.ds(0, cols)], ya_s, ya_r.at[0], yn).wait_send()
    wait_s1(0)
    with scope("rescale"):
        loop(0, nh, lambda i: rescale(0, nh - 1 - i))

    near = nc * WIDTH

    def put(n, v):
        v = v * v
        c1[n] = v
        parts[n] = fold(v)

    def last_near(n):
        c1[n] = dot(a0[:, :cols], gown[n, :half, :])

    def last_other(n):
        c1[n] += dot(a0[:, cols:near], gown[n, half:near, :])

    def last(n):
        c1[n] = dot(a0[:, :near], gown[n, :near, :])

    def last_far(i):
        put(2 * i, c1[2 * i] + dot(a2[...], gown[2 * i, near:, :]))
        put(2 * i + 1, c1[2 * i + 1] + dot(a2[...], gown[2 * i + 1, near:, :]))

    def last_whole(n):
        put(n, dot(a0[:, :near], gown[n, :near, :]) + dot(a2[...], gown[n, near:, :]))
    with scope("last_near"):
        remote(a0.at[:, lent], a2, y2_s, y2_r, yn).start()
        loop(0, 2, last_near)
    wait_s1(1)
    with scope("rescale"):
        loop(0, nf, lambda n: rescale(1, n))
    with scope("last"):
        loop(0, 2, last_other)
        loop(2, nh - 2, last)
    with scope("wait_a2"):
        remote(a0.at[:, lent], a2, y2_s, y2_r, yn).wait()
    with scope("last_far"):
        loop(0, (nh - 2) // 2, last_far)
    with scope("last_whole"):
        loop(nh - 2, nh, last_whole)
        s2[r] = jnp.sum(parts[:nh], axis=1)

    for dev in (cn, xn, dn):
        remote(s2.at[r], s2.at[r], s2_s, s2_r, dev).start()

    def sent(ref, sem):
        remote(ref, ref, sem, s2_r, cn).wait_send()
    sent(gown.at[:, pl.ds(0, rows)], xown_s)
    sent(gown.at[pl.ds(0, nf), pl.ds(0, rows)], yg_s)
    sent(gown.at[:, pl.ds(0, rows)], cown_s)
    sent(gown.at[pl.ds(0, nf), pl.ds(0, rows)], xfwd_s)
    sent(gown.at[:, pl.ds(0, rows)], cfwd_s)
    sent(gown.at[pl.ds(0, nf), pl.ds(0, 2 * rows)], cfar_s)
    sent(sums.at[:, pl.ds(0, 3)], sum_s)
    sent(s1.at[:, pl.ds(0, 3)], s1_s)
    with scope("wait_s2"):
        three = s2.at[pl.ds(0, 3)]
        remote(three, three, s2_s, s2_r, cn).wait()
    total = (s2[0] + s2[1]) + (s2[2] + s2[3])
    for n in range(nh):
        sum_ref[:, n * WIDTH:(n + 1) * WIDTH] = total[n:n + 1]


def scale_kernel(n_all, raw_ref, sum_ref, out_ref, buf, out_sem):
    def put(i):
        return pltpu.make_async_copy(buf.at[i], out_ref.at[:, pl.ds(i * WIDTH, WIDTH)], out_sem.at[i])

    chunks = raw_ref.shape[0]
    for i in range(chunks):
        buf[i] = raw_ref[i] * (n_all / sum_ref[:, i * WIDTH:(i + 1) * WIDTH])
        put(i).start()
    for i in range(chunks):
        put(i).wait()


def solution(mesh):
    block_spec = P(("graph", "row"), "col")

    def device_step(init_blk, graph_blk):
        rows, cols = init_blk.shape
        n_all = 2 * cols
        nh = cols // WIDTH
        dma = pltpu.SemaphoreType.DMA
        any_spec, vmem_spec = pl.BlockSpec(memory_space=pl.ANY), pl.BlockSpec(memory_space=pltpu.VMEM)
        raw, col_sum, _ = pl.pallas_call(
            functools.partial(kernel, float(n_all)),
            out_shape=(
                pltpu.VMEM((nh, rows, WIDTH), F32),
                pltpu.VMEM((1, cols), F32),
                jax.ShapeDtypeStruct((nh - 1, n_all, WIDTH), BF16),
            ),
            in_specs=[any_spec, any_spec],
            out_specs=(vmem_spec, vmem_spec, any_spec),
            scratch_shapes=[
                pltpu.VMEM((rows, n_all), BF16),
                pltpu.VMEM((rows, n_all), BF16),
                pltpu.VMEM((rows, WIDTH), BF16),
                pltpu.VMEM((nh, rows, WIDTH), F32),
                pltpu.VMEM((2, rows, WIDTH), F32),
                pltpu.VMEM((nh, n_all, WIDTH), BF16),
                pltpu.VMEM((2, n_all, WIDTH), BF16),
                pltpu.VMEM((nh, 2 * WIDTH, WIDTH), BF16),
                pltpu.VMEM((2 * nh - 1, 4, 1, WIDTH), F32),
                pltpu.VMEM((2, 4, nh, WIDTH), F32),
                pltpu.VMEM((4, nh, WIDTH), F32),
                pltpu.VMEM((2 * nh, 8, WIDTH), F32),
                dma((2 * nh,)), dma((2,)), dma((nh,)),
                dma((nh,)), dma((nh, PIECES)), dma((2,)), dma((nh, PIECES)), dma, dma,
                dma((2 * nh,)), dma((2 * nh,)), dma((2,)), dma,
                dma, dma, dma, dma, dma, dma, dma, dma, dma, dma, dma, dma,
            ],
            compiler_params=pltpu.CompilerParams(
                collective_id=0, has_side_effects=True, vmem_limit_bytes=54 * 2**20),
            name="mcl",
        )(init_blk, graph_blk)
        return pl.pallas_call(
            functools.partial(scale_kernel, float(n_all)),
            out_shape=jax.ShapeDtypeStruct((rows, cols), F32),
            in_specs=[vmem_spec, vmem_spec],
            out_specs=any_spec,
            scratch_shapes=[pltpu.VMEM((nh, rows, WIDTH), F32), dma((nh,))],
            compiler_params=pltpu.CompilerParams(vmem_limit_bytes=40 * 2**20),
            name="scale",
        )(raw, col_sum)

    return jax.shard_map(device_step, mesh=mesh, in_specs=(block_spec, block_spec), out_specs=block_spec, check_vma=False)
```
